32 devices in a mesh: fsdp: 8 (over y, x, core), tp: 4 (over z).
Axes of the slice: x: 2, y: 2, z: 4, core: 2. Of those that a mesh axis runs over, the one named last changes fastest.
Arguments:
- tokens: bfloat16 [4096, 2048], P(('fsdp', 'tp')), may hold values from -6 to 6
- attention_norm_gain: bfloat16 [2048], P(('fsdp', 'tp')), may hold values from 0.5 to 1.5
- feedforward_norm_gain: bfloat16 [2048], P(('fsdp', 'tp')), may hold values from 0.5 to 1.5
- query_shared_weight: bfloat16 [2048, 2048], P('fsdp', 'tp'), may hold values from -0.125 to 0.125
- key_value_shared_weight: bfloat16 [2048, 512], P(('fsdp', 'tp')), may hold values from -0.125 to 0.125
- output_shared_weight: bfloat16 [2048, 2048], P('tp', 'fsdp'), may hold values from -0.75 to 0.75
- gate_shared_weight: bfloat16 [2048, 16384], P('fsdp', 'tp'), may hold values from -0.125 to 0.125
- up_shared_weight: bfloat16 [2048, 16384], P('fsdp', 'tp'), may hold values from -0.125 to 0.125
- down_shared_weight: bfloat16 [16384, 2048], P('tp', 'fsdp'), may hold values from -0.046875 to 0.046875
- attention_delta_input: bfloat16 [2048, 256], P(('fsdp', 'tp')), may hold values from -0.125 to 0.125
- query_delta_output: bfloat16 [256, 2048], P('fsdp', 'tp'), may hold values from -0.375 to 0.375
- key_value_delta_output: bfloat16 [256, 512], P(('fsdp', 'tp')), may hold values from -0.375 to 0.375
- output_delta_input: bfloat16 [2048, 256], P('tp', 'fsdp'), may hold values from -0.125 to 0.125
- output_delta_output: bfloat16 [256, 2048], P(('fsdp', 'tp')), may hold values from -2 to 2
- feedforward_delta_input: bfloat16 [2048, 256], P(('fsdp', 'tp')), may hold values from -0.125 to 0.125
- gate_delta_output: bfloat16 [256, 16384], P('fsdp', 'tp'), may hold values from -0.375 to 0.375
- up_delta_output: bfloat16 [256, 16384], P('fsdp', 'tp'), may hold values from -0.375 to 0.375
- down_delta_input: bfloat16 [16384, 256], P('tp', 'fsdp'), may hold values from -0.046875 to 0.046875
- down_delta_output: bfloat16 [256, 2048], P(('fsdp', 'tp')), may hold values from -0.375 to 0.375
- picture_begin_index: int32 [4], replicated, may hold values from 257 to 511
- cotangent: bfloat16 [4096, 2048], P(('fsdp', 'tp')), may hold values from -6 to 6
Outputs:
- result: bfloat16 [4096, 2048], P(('fsdp', 'tp'))
- tokens_grad: float32 [4096, 2048], P(('fsdp', 'tp'))
- attn_gain_grad: float32 [2048], P(('fsdp', 'tp'))
- mlp_gain_grad: float32 [2048], P(('fsdp', 'tp'))
- query_weight_grad: float32 [2048, 2048], P('fsdp', 'tp')
- keyval_weight_grad: float32 [2048, 512], P(('fsdp', 'tp'))
- out_weight_grad: float32 [2048, 2048], P('tp', 'fsdp')
- gate_weight_grad: float32 [2048, 16384], P('fsdp', 'tp')
- up_weight_grad: float32 [2048, 16384], P('fsdp', 'tp')
- down_weight_grad: float32 [16384, 2048], P('tp', 'fsdp')
- attn_lora_in_grad: float32 [2048, 256], P(('fsdp', 'tp'))
- query_lora_out_grad: float32 [256, 2048], P('fsdp', 'tp')
- keyval_lora_out_grad: float32 [256, 512], P(('fsdp', 'tp'))
- out_lora_in_grad: float32 [2048, 256], P('tp', 'fsdp')
- out_lora_out_grad: float32 [256, 2048], P(('fsdp', 'tp'))
- mlp_lora_in_grad: float32 [2048, 256], P(('fsdp', 'tp'))
- gate_lora_out_grad: float32 [256, 16384], P('fsdp', 'tp')
- up_lora_out_grad: float32 [256, 16384], P('fsdp', 'tp')
- down_lora_in_grad: float32 [16384, 256], P('tp', 'fsdp')
- down_lora_out_grad: float32 [256, 2048], P(('fsdp', 'tp'))
The draws below stay inside these ranges and needn't reach their ends.
All inputs are finite; a program needn't handle non-finite values.
Results may differ from the reference program's by a relative error of at most 0.017.
The reference program's roundings to bfloat16 on the way count: a program that leaves them out, or rounds other values in their place, can miss the bound.
Values may be sent and summed in bfloat16 or wider, within the bound.
A program may use at most 320 MiB of HBM per device.

```python
import jax
import jax.numpy as jnp
from jax import lax

MODEL_WIDTH = 2048
QUERY_HEADS = 8
HEAD_WIDTH = 256
HIDDEN_UNITS = 16384
DELTA_RANK = 256
PICTURE = 256
SEQ = 1024
SEQS = 4
TOKENS = 4096


def with_ends(result, key, least, high):
    spot = [jax.random.randint(jax.random.fold_in(key, axis), (), 0, length) for axis, length in enumerate(result.shape)]
    main_axis = result.shape.index(max(result.shape))
    next_to = spot[:main_axis] + [(spot[main_axis] + 1) % result.shape[main_axis]] + spot[main_axis + 1:]
    return result.at[tuple(spot)].set(least).at[tuple(next_to)].set(high)


def levels(key, extent, pieces, least, high):
    factor_of, own = 1.0, jax.random.fold_in(key, 6)
    for axis_at, parts in pieces:
        heights = jnp.exp(jax.random.uniform(jax.random.fold_in(own, axis_at), (parts,), jnp.float32, least / len(pieces), high / len(pieces)))
        factor_of = factor_of * jnp.repeat(heights, extent[axis_at] // parts).reshape([-1 if axis == axis_at else 1 for axis in range(len(extent))])
    return factor_of


def bell_draw(stream_key, shape, scale, bound, split=(), kind=jnp.bfloat16):
    result = jax.random.normal(stream_key, shape, jnp.float32) * scale
    if len(split) > 0:
        result = levels(stream_key, shape, split, -0.22, 0.18) * result
    return jnp.clip(result, min=-bound, max=bound).astype(kind)


def setup_inputs(seed: int = 0) -> dict:
    key_list = jax.random.split(jax.random.key(seed), 22)
    tokens = bell_draw(key_list[0], (TOKENS, MODEL_WIDTH), 1.0, 6.0, ((0, 32),))
    attention_norm_gain = jnp.clip(1.0 + 0.1 * jax.random.normal(key_list[1], (MODEL_WIDTH,), jnp.float32), 0.5, 1.5).astype(jnp.bfloat16)
    feedforward_norm_gain = jnp.clip(1.0 + 0.1 * jax.random.normal(key_list[2], (MODEL_WIDTH,), jnp.float32), 0.5, 1.5).astype(jnp.bfloat16)
    query_shared_weight = bell_draw(key_list[3], (MODEL_WIDTH, QUERY_HEADS * HEAD_WIDTH), MODEL_WIDTH ** -0.5, 0.125, ((0, 8), (1, 4)))
    key_value_shared_weight = bell_draw(key_list[4], (MODEL_WIDTH, 2 * HEAD_WIDTH), MODEL_WIDTH ** -0.5, 0.125, ((0, 32),))
    output_shared_weight = bell_draw(key_list[5], (QUERY_HEADS * HEAD_WIDTH, MODEL_WIDTH), 64 ** -0.5, 0.75, ((0, 4), (1, 8)))
    gate_shared_weight = bell_draw(key_list[6], (MODEL_WIDTH, HIDDEN_UNITS), MODEL_WIDTH ** -0.5, 0.125, ((0, 8), (1, 4)))
    up_shared_weight = bell_draw(key_list[7], (MODEL_WIDTH, HIDDEN_UNITS), MODEL_WIDTH ** -0.5, 0.125, ((0, 8), (1, 4)))
    down_shared_weight = bell_draw(key_list[8], (HIDDEN_UNITS, MODEL_WIDTH), HIDDEN_UNITS ** -0.5, 0.046875, ((0, 4), (1, 8)))
    attention_delta_input = bell_draw(key_list[9], (MODEL_WIDTH, DELTA_RANK), MODEL_WIDTH ** -0.5, 0.125, ((0, 32),))
    query_delta_output = bell_draw(key_list[10], (DELTA_RANK, QUERY_HEADS * HEAD_WIDTH), DELTA_RANK ** -0.5, 0.375, ((0, 8), (1, 4)))
    key_value_delta_output = bell_draw(key_list[11], (DELTA_RANK, 2 * HEAD_WIDTH), DELTA_RANK ** -0.5, 0.375, ((0, 32),))
    output_delta_input = bell_draw(key_list[12], (QUERY_HEADS * HEAD_WIDTH, DELTA_RANK), (QUERY_HEADS * HEAD_WIDTH) ** -0.5, 0.125, ((0, 4), (1, 8)))
    output_delta_output = bell_draw(key_list[13], (DELTA_RANK, MODEL_WIDTH), 8 ** -0.5, 2.0, ((0, 32),))
    feedforward_delta_input = bell_draw(key_list[14], (MODEL_WIDTH, DELTA_RANK), MODEL_WIDTH ** -0.5, 0.125, ((0, 32),))
    gate_delta_output = bell_draw(key_list[15], (DELTA_RANK, HIDDEN_UNITS), DELTA_RANK ** -0.5, 0.375, ((0, 8), (1, 4)))
    up_delta_output = bell_draw(key_list[16], (DELTA_RANK, HIDDEN_UNITS), DELTA_RANK ** -0.5, 0.375, ((0, 8), (1, 4)))
    down_delta_input = bell_draw(key_list[17], (HIDDEN_UNITS, DELTA_RANK), HIDDEN_UNITS ** -0.5, 0.046875, ((0, 4), (1, 8)))
    down_delta_output = bell_draw(key_list[18], (DELTA_RANK, MODEL_WIDTH), DELTA_RANK ** -0.5, 0.375, ((0, 32),))
    picture_begin_index = with_ends(jax.random.randint(key_list[19], (SEQS,), SEQ // 2 - PICTURE + 1, SEQ // 2), jax.random.fold_in(key_list[19], 1), SEQ // 2 - PICTURE + 1, (SEQ // 2) - 1).astype(jnp.int32)
    cotangent = bell_draw(key_list[20], (TOKENS, MODEL_WIDTH), 1.0, 6.0, ((0, 32),))
    return dict(tokens=tokens, attention_norm_gain=attention_norm_gain, feedforward_norm_gain=feedforward_norm_gain, query_shared_weight=query_shared_weight, key_value_shared_weight=key_value_shared_weight, output_shared_weight=output_shared_weight, gate_shared_weight=gate_shared_weight, up_shared_weight=up_shared_weight, down_shared_weight=down_shared_weight, attention_delta_input=attention_delta_input, query_delta_output=query_delta_output, key_value_delta_output=key_value_delta_output, output_delta_input=output_delta_input, output_delta_output=output_delta_output, feedforward_delta_input=feedforward_delta_input, gate_delta_output=gate_delta_output, up_delta_output=up_delta_output, down_delta_input=down_delta_input, down_delta_output=down_delta_output, picture_begin_index=picture_begin_index, cotangent=cotangent)


@jax.custom_vjp
def reduced_precision(v):
    return lax.optimization_barrier(v.astype(jnp.bfloat16)).astype(jnp.float32)

@jax.custom_vjp
def low_back(v):
    return v

def low_keep(v):
    return (reduced_precision(v), None)

def low_pass(kept, grad):
    return (grad,)

def back_keep(v):
    return (v, None)

def back_low(kept, grad):
    return (reduced_precision(grad),)
reduced_precision.defvjp(low_keep, low_pass)
low_back.defvjp(back_keep, back_low)
EPSILON = 1e-06
EXACT = lax.Precision.HIGHEST

def matrix_product(left_mat, right_mat):
    return jnp.dot(left_mat, right_mat, precision=EXACT)

def normalize(values, gain_vec):
    return values * lax.rsqrt(lax.optimization_barrier(jnp.mean(values * values, axis=-1, keepdims=True)) + EPSILON) * gain_vec

def rotate(values, positions):
    half_dim = HEAD_WIDTH // 2
    frequency = 10000.0 ** (-2.0 * jnp.arange(half_dim, dtype=jnp.float32) / HEAD_WIDTH)
    angles = positions.astype(jnp.float32)[:, None] * frequency[None, :]
    cosine = jnp.cos(angles)[:, None, :]
    sine_part = jnp.sin(angles)[:, None, :]
    first_half = values[..., :half_dim]
    second = values[..., half_dim:]
    return jnp.concatenate([first_half * cosine - second * sine_part, second * cosine + first_half * sine_part], axis=-1)

def one_sequence(inputs, picture_at, weight_bundle):
    query_eff, keyval_eff, out_eff, gate_combined, up_combined, down_combined, gain_attn, gain_mlp = weight_bundle
    positions = jnp.arange(SEQ, dtype=jnp.int32)
    normed = reduced_precision(normalize(inputs, gain_attn))
    query_lin = low_back(matrix_product(normed, query_eff)).reshape(SEQ, QUERY_HEADS, HEAD_WIDTH)
    keyval_lin = low_back(matrix_product(normed, keyval_eff))
    queries = reduced_precision(rotate(query_lin, positions) * HEAD_WIDTH ** (-0.5))
    keys = reduced_precision(rotate(keyval_lin[:, None, :HEAD_WIDTH], positions))[:, 0, :]
    values = reduced_precision(keyval_lin[:, HEAD_WIDTH:])
    scores = low_back(jnp.einsum('shd,td->hst', queries, keys, precision=EXACT))
    inside = (positions >= picture_at) & (positions < picture_at + PICTURE)
    allowed = (positions[None, :] <= positions[:, None]) | inside[:, None] & inside[None, :]
    probabilities = jax.nn.softmax(jnp.where(allowed[None], scores, -1e+30), axis=-1)
    mixed_heads = jnp.einsum('hst,td->shd', reduced_precision(probabilities), values, precision=EXACT)
    mixed_heads = reduced_precision(low_back(mixed_heads.reshape(SEQ, QUERY_HEADS * HEAD_WIDTH)))
    hidden = inputs + low_back(matrix_product(mixed_heads, out_eff))
    normed_mlp = reduced_precision(normalize(hidden, gain_mlp))
    gate_lin = low_back(matrix_product(normed_mlp, gate_combined))
    up_lin = low_back(matrix_product(normed_mlp, up_combined))
    activation = reduced_precision(jax.nn.gelu(gate_lin, approximate=True) * up_lin)
    return hidden + low_back(matrix_product(activation, down_combined))

def forward_layer(tokens, attention_norm_gain, feedforward_norm_gain, query_shared_weight, key_value_shared_weight, output_shared_weight, gate_shared_weight, up_shared_weight, down_shared_weight, attention_delta_input, query_delta_output, key_value_delta_output, output_delta_input, output_delta_output, feedforward_delta_input, gate_delta_output, up_delta_output, down_delta_input, down_delta_output, picture_begin_index):
    weight_bundle = (reduced_precision(query_shared_weight + matrix_product(attention_delta_input, query_delta_output)), reduced_precision(key_value_shared_weight + matrix_product(attention_delta_input, key_value_delta_output)), reduced_precision(output_shared_weight + matrix_product(output_delta_input, output_delta_output)), reduced_precision(gate_shared_weight + matrix_product(feedforward_delta_input, gate_delta_output)), reduced_precision(up_shared_weight + matrix_product(feedforward_delta_input, up_delta_output)), reduced_precision(down_shared_weight + matrix_product(down_delta_input, down_delta_output)), attention_norm_gain, feedforward_norm_gain)
    sequences = tokens.reshape(SEQS, SEQ, MODEL_WIDTH)

    def one_item(item):
        return one_sequence(item[0], item[1], weight_bundle)
    outputs = lax.map(jax.checkpoint(one_item), (sequences, picture_begin_index))
    return outputs.reshape(SEQS * SEQ, MODEL_WIDTH)

def reference(tokens, attention_norm_gain, feedforward_norm_gain, query_shared_weight, key_value_shared_weight, output_shared_weight, gate_shared_weight, up_shared_weight, down_shared_weight, attention_delta_input, query_delta_output, key_value_delta_output, output_delta_input, output_delta_output, feedforward_delta_input, gate_delta_output, up_delta_output, down_delta_input, down_delta_output, picture_begin_index, cotangent):
    float_values = [numeric_array.astype(jnp.float32) for numeric_array in (tokens, attention_norm_gain, feedforward_norm_gain, query_shared_weight, key_value_shared_weight, output_shared_weight, gate_shared_weight, up_shared_weight, down_shared_weight, attention_delta_input, query_delta_output, key_value_delta_output, output_delta_input, output_delta_output, feedforward_delta_input, gate_delta_output, up_delta_output, down_delta_input, down_delta_output)]
    output, pullback = jax.vjp(lambda *arrays: forward_layer(*arrays, picture_begin_index), *float_values)
    gradients = pullback(cotangent.astype(jnp.float32))
    return (output.astype(jnp.bfloat16), gradients[0], gradients[1], gradients[2], gradients[3], gradients[4], gradients[5], gradients[6], gradients[7], gradients[8], gradients[9], gradients[10], gradients[11], gradients[12], gradients[13], gradients[14], gradients[15], gradients[16], gradients[17], gradients[18])
```

```python
import jax
import jax.numpy as jnp
from jax import lax
from jax.sharding import PartitionSpec as P

HEAD_WIDTH = 256
PICTURE = 256


EPSILON = 1e-06
BLOCK_ROWS = 512


def partner(value, axis, apart):
    mask = 2**apart
    pairs = [(source, source ^ mask) for source in range(lax.axis_size(axis))]
    return lax.ppermute(value, axis, pairs)


def matrix_multiply(left_mat, right_mat):
    return jnp.dot(left_mat, right_mat, preferred_element_type=jnp.float32)


def times_transposed(left_mat, right_mat):
    return lax.dot_general(
        left_mat, right_mat, (((1,), (1,)), ((), ())), preferred_element_type=jnp.float32
    )


def transposed_times(left_mat, right_mat):
    return lax.dot_general(
        left_mat, right_mat, (((0,), (0,)), ((), ())), preferred_element_type=jnp.float32
    )


def merged_weight(shared_base, delta_left_factor, delta_right_factor):
    return (
        shared_base.astype(jnp.float32) + matrix_multiply(delta_left_factor, delta_right_factor)
    ).astype(jnp.bfloat16)


def normalize(values, gain_vec):
    return (
        values * lax.rsqrt(jnp.mean(values * values, axis=-1, keepdims=True) + EPSILON) * gain_vec
    )


def rotate(values, positions, direction):
    half_dim = HEAD_WIDTH // 2
    frequency = 10000.0 ** (-2.0 * jnp.arange(half_dim, dtype=jnp.float32) / HEAD_WIDTH)
    angles = positions.astype(jnp.float32)[:, None] * frequency[None, :]
    cosine = jnp.cos(angles)[:, None, :]
    sine_part = direction * jnp.sin(angles)[:, None, :]
    first_half = values[..., :half_dim]
    second = values[..., half_dim:]
    return jnp.concatenate(
        [first_half * cosine - second * sine_part, second * cosine + first_half * sine_part],
        axis=-1,
    )


def allowed_mask(query_pos, key_pos, picture_at):
    inside_query = (query_pos >= picture_at) & (query_pos < picture_at + PICTURE)
    inside_key = (key_pos >= picture_at) & (key_pos < picture_at + PICTURE)
    return (key_pos[None, :] <= query_pos[:, None]) | inside_query[:, None] & inside_key[None, :]


def joined(axis_names, value, axis=0):
    return lax.all_gather(value, axis_names, axis=axis, tiled=True)


def scattered(axis_names, value):
    return lax.psum_scatter(value, axis_names, scatter_dimension=0, tiled=True)


def low(value):
    return value.astype(jnp.bfloat16)


def to_lanes(value, width):
    return jnp.concatenate(
        [value[:, at : at + width] for at in range(0, value.shape[1], width)], axis=0
    )


class Packed:
    def __init__(self, width):
        self.width, self.pieces, self.shapes = width, [], []

    def add(self, value):
        self.shapes.append(value.shape)
        self.pieces.append(to_lanes(value, self.width))

    def gather(self, axis_names):
        whole = lax.all_gather(jnp.concatenate(self.pieces, axis=0), axis_names, axis=0)
        results, at = [], 0
        for rows, columns in self.shapes:
            parts = []
            for _ in range(columns // self.width):
                parts.append(whole[:, at : at + rows].reshape(-1, self.width))
                at += rows
            results.append(jnp.concatenate(parts, axis=1))
        return results


def blocked(main_cols, extra_cols, parts):
    rows = main_cols.shape[0]
    return jnp.concatenate(
        [main_cols.reshape(rows, parts, -1), extra_cols.reshape(rows, parts, -1)], axis=2
    ).reshape(rows, -1)


def shards(
    tokens,
    attention_norm_gain,
    feedforward_norm_gain,
    query_shared_weight,
    key_value_shared_weight,
    output_shared_weight,
    gate_shared_weight,
    up_shared_weight,
    down_shared_weight,
    attention_delta_input,
    query_delta_output,
    key_value_delta_output,
    output_delta_input,
    output_delta_output,
    feedforward_delta_input,
    gate_delta_output,
    up_delta_output,
    down_delta_input,
    down_delta_output,
    picture_begin_index,
    cotangent,
):
    both = ("fsdp", "tp")
    tp_size = lax.axis_size("tp")
    fsdp_size = lax.axis_size("fsdp")
    parts = tp_size * fsdp_size
    own_rows, model_width = tokens.shape
    span_rows = own_rows * tp_size
    key_rows = 2 * span_rows
    block_rows = min(BLOCK_ROWS, span_rows)
    block_count = span_rows // block_rows
    placed = lax.axis_index("fsdp")
    tp_at = lax.axis_index("tp")
    second_half = placed % 2
    picture_at = lax.dynamic_slice_in_dim(picture_begin_index, placed // 2, 1)[0]
    offset_rows = second_half * span_rows
    span_positions = offset_rows + jnp.arange(span_rows, dtype=jnp.int32)
    key_positions = jnp.arange(key_rows, dtype=jnp.int32)
    scaling = HEAD_WIDTH ** (-0.5)

    rank = gate_delta_output.shape[0] * fsdp_size
    common = Packed(rank)
    gain_rows = jnp.concatenate([attention_norm_gain[None], feedforward_norm_gain[None]], axis=0)
    common.add(jnp.pad(gain_rows, ((0, 6), (0, rank - gain_rows.shape[1]))))
    common.add(key_value_shared_weight)
    common.add(attention_delta_input)
    common.add(key_value_delta_output)
    common.add(output_delta_output)
    common.add(feedforward_delta_input)
    common.add(down_delta_output)
    (
        gains,
        key_value_complete,
        delta_attention,
        key_value_delta_product,
        output_delta_product,
        delta_feedforward,
        down_delta_product,
    ) = common.gather(both)
    gains = gains.reshape(parts, 8, rank)[:, :2, : gain_rows.shape[1]].astype(jnp.float32)
    gain_attn = gains[:, 0].reshape(-1)
    gain_mlp = gains[:, 1].reshape(-1)

    rows_both = joined("tp", jnp.concatenate([tokens, cotangent], axis=1))
    tokens_span = rows_both[:, :model_width]
    grad_span = rows_both[:, model_width:]

    width = output_shared_weight.shape[1]
    heads_pack = Packed(width)
    heads_pack.add(query_shared_weight)
    heads_pack.add(query_delta_output)
    heads_pack.add(output_delta_input.T)
    heads_pack.add(output_shared_weight)
    query_complete, query_delta_product, out_down_t, out_stack = heads_pack.gather("fsdp")
    out_rows = output_shared_weight.shape[0]
    out_full = (
        out_stack.reshape(fsdp_size, out_rows, width).transpose(1, 0, 2).reshape(out_rows, -1)
    )
    query_eff = merged_weight(query_complete, delta_attention, query_delta_product)
    keyval_eff = merged_weight(key_value_complete, delta_attention, key_value_delta_product)
    out_eff = low(out_full.astype(jnp.float32) + transposed_times(out_down_t, output_delta_product))

    delta_rows = gate_delta_output.shape[0]
    delta_stack = lax.all_gather(
        jnp.concatenate([gate_delta_output, up_delta_output, down_delta_input.T], axis=0),
        "fsdp",
        axis=0,
    )
    gate_delta_product, up_delta_product, down_in_t = (
        delta_stack[:, at * delta_rows : (at + 1) * delta_rows].reshape(rank, -1) for at in range(3)
    )
    shard_rows = gate_shared_weight.shape[0]
    delta_feedforward_rows = lax.dynamic_slice_in_dim(
        delta_feedforward, placed * shard_rows, shard_rows
    )
    down_delta_cols = lax.dynamic_slice_in_dim(
        down_delta_product, placed * shard_rows, shard_rows, axis=1
    )
    down_eff = joined(
        "fsdp",
        low(
            down_shared_weight.astype(jnp.float32) + transposed_times(down_in_t, down_delta_cols)
        ),
        axis=1,
    )
    gate_eff = joined(
        "fsdp", merged_weight(gate_shared_weight, delta_feedforward_rows, gate_delta_product)
    )
    up_eff = joined(
        "fsdp", merged_weight(up_shared_weight, delta_feedforward_rows, up_delta_product)
    )

    inputs = tokens.astype(jnp.float32)
    inputs_span = tokens_span.astype(jnp.float32)
    normed_span = low(normalize(inputs_span, gain_attn))
    keyval_span = matrix_multiply(normed_span, keyval_eff)
    keys_span = rotate(keyval_span[:, None, :HEAD_WIDTH], span_positions, 1.0)[:, 0, :]
    keyval_low = low(jnp.concatenate([keys_span, keyval_span[:, HEAD_WIDTH:]], axis=1))
    keyval_other = partner(keyval_low, "fsdp", 0)
    keyval_all = jnp.where(
        second_half == 1,
        jnp.concatenate([keyval_other, keyval_low], axis=0),
        jnp.concatenate([keyval_low, keyval_other], axis=0),
    )
    keys_all = keyval_all[:, :HEAD_WIDTH]
    values_all = keyval_all[:, HEAD_WIDTH:]
    query_lin = matrix_multiply(normed_span, query_eff)
    local_heads = query_lin.shape[1] // HEAD_WIDTH
    query_rot = (
        rotate(query_lin.reshape(span_rows, local_heads, HEAD_WIDTH), span_positions, 1.0) * scaling
    )
    query_blocks = (
        low(query_rot)
        .transpose(1, 0, 2)
        .reshape(local_heads * block_count, block_rows, HEAD_WIDTH)
    )

    def block_mask(block_index):
        query_pos = (
            offset_rows
            + block_index % block_count * block_rows
            + jnp.arange(block_rows, dtype=jnp.int32)
        )
        return allowed_mask(query_pos, key_positions, picture_at)

    def attend(block_index):
        query_rows = query_blocks[block_index]
        scores = jnp.where(block_mask(block_index), times_transposed(query_rows, keys_all), -1e30)
        maximum = jnp.max(scores, axis=-1, keepdims=True)
        exponent = jnp.exp(scores - maximum)
        normalizer = jnp.sum(exponent, axis=-1, keepdims=True)
        probabilities = low(exponent / normalizer)
        return (matrix_multiply(probabilities, values_all), (maximum + jnp.log(normalizer))[:, 0])

    block_ids = jnp.arange(local_heads * block_count, dtype=jnp.int32)
    mixed_blocks, log_totals = lax.map(attend, block_ids)
    mixed_heads = low(
        mixed_blocks.reshape(local_heads, span_rows, HEAD_WIDTH)
        .transpose(1, 0, 2)
        .reshape(span_rows, local_heads * HEAD_WIDTH)
    )
    attn_result = scattered("tp", low(matrix_multiply(mixed_heads, out_eff)))
    hidden = inputs + attn_result.astype(jnp.float32)
    normed_mlp = joined("tp", low(normalize(hidden, gain_mlp)))

    grad_activation = times_transposed(grad_span, down_eff)
    gate_lin = matrix_multiply(normed_mlp, gate_eff)
    up_lin = matrix_multiply(normed_mlp, up_eff)
    activation, gelu_pull = jax.vjp(
        lambda gate_vals, up_vals: jax.nn.gelu(gate_vals, approximate=True) * up_vals,
        gate_lin,
        up_lin,
    )
    activation = low(activation)
    grad_gate, grad_up = gelu_pull(grad_activation)
    grad_gate, grad_up = low(grad_gate), low(grad_up)
    grad_normed_mlp = scattered(
        "tp",
        low(times_transposed(grad_gate, gate_eff) + times_transposed(grad_up, up_eff)),
    ).astype(jnp.float32)
    _, mlp_norm_pull = jax.vjp(normalize, hidden, gain_mlp)
    grad_hidden_norm, mlp_gain_part = mlp_norm_pull(grad_normed_mlp)
    grad_hidden = cotangent.astype(jnp.float32) + grad_hidden_norm
    grad_hidden_span = joined("tp", low(grad_hidden))
    mlp_result = scattered("tp", low(matrix_multiply(activation, down_eff)))
    result = low(hidden + mlp_result.astype(jnp.float32))

    normed_delta = low(matrix_multiply(normed_mlp, delta_feedforward))
    normed_wide = blocked(normed_mlp, normed_delta, fsdp_size)
    grad_delta = low(times_transposed(grad_span, down_delta_product))
    grad_wide = blocked(grad_span, grad_delta, fsdp_size)
    down_sum = scattered("fsdp", low(transposed_times(grad_wide, activation)))
    gate_sum = scattered("fsdp", low(transposed_times(normed_wide, grad_gate)))
    up_sum = scattered("fsdp", low(transposed_times(normed_wide, grad_up)))
    mlp_inner = low(
        times_transposed(grad_gate, gate_delta_product)
        + times_transposed(grad_up, up_delta_product)
    )
    mlp_lora_in = low(transposed_times(normed_mlp, mlp_inner))
    active_delta = low(times_transposed(activation, down_in_t))
    down_lora_out = low(transposed_times(active_delta, grad_span))

    grad_mixed = low(times_transposed(grad_hidden_span, out_eff))
    grad_blocks = (
        grad_mixed.reshape(span_rows, local_heads, HEAD_WIDTH)
        .transpose(1, 0, 2)
        .reshape(local_heads * block_count, block_rows, HEAD_WIDTH)
    )

    def revisit(totals, block_index):
        key_totals, value_totals = totals
        query_rows = query_blocks[block_index]
        grad_rows = grad_blocks[block_index]
        scores = jnp.where(block_mask(block_index), times_transposed(query_rows, keys_all), -1e30)
        probabilities = jnp.exp(scores - log_totals[block_index][:, None])
        grad_probs = times_transposed(grad_rows, values_all)
        inner_sum = jnp.sum(probabilities * grad_probs, axis=-1, keepdims=True)
        grad_scores = low(probabilities * (grad_probs - inner_sum))
        key_totals = key_totals + transposed_times(grad_scores, query_rows)
        value_totals = value_totals + transposed_times(low(probabilities), grad_rows)
        return ((key_totals, value_totals), matrix_multiply(grad_scores, keys_all))

    zero_rows = jnp.zeros((key_rows, HEAD_WIDTH), jnp.float32)
    (key_totals, value_totals), grad_query_blocks = lax.scan(
        revisit, (zero_rows, zero_rows), block_ids
    )
    grad_queries = (
        grad_query_blocks.reshape(local_heads, span_rows, HEAD_WIDTH).transpose(1, 0, 2) * scaling
    )
    grad_query_lin = low(
        rotate(grad_queries, span_positions, -1.0).reshape(span_rows, local_heads * HEAD_WIDTH)
    )
    keyval_totals = jnp.concatenate([key_totals, value_totals], axis=1)
    lower_rows = keyval_totals[:span_rows]
    upper_rows = keyval_totals[span_rows:]
    mine = jnp.where(second_half == 1, upper_rows, lower_rows)
    theirs = jnp.where(second_half == 1, lower_rows, upper_rows)
    keyval_part = mine + partner(theirs, "fsdp", 0)
    grad_keys = rotate(keyval_part[:, None, :HEAD_WIDTH], span_positions, -1.0)[:, 0, :]
    grad_keyval = low(jnp.concatenate([grad_keys, keyval_part[:, HEAD_WIDTH:]], axis=1))
    grad_normed_part = times_transposed(grad_query_lin, query_eff) + times_transposed(
        grad_keyval, keyval_eff
    )
    grad_normed_attn = scattered("tp", low(grad_normed_part)).astype(jnp.float32)
    unit_span = inputs_span * lax.rsqrt(
        jnp.mean(inputs_span * inputs_span, axis=-1, keepdims=True) + EPSILON
    )
    attn_gain_part = jnp.sum(grad_normed_part * unit_span, axis=0)
    _, attn_norm_pull = jax.vjp(normalize, inputs, gain_attn)
    tokens_grad = grad_hidden + attn_norm_pull(grad_normed_attn)[0]

    mixed_delta = low(times_transposed(mixed_heads, out_down_t))
    out_lora_out = low(transposed_times(mixed_delta, grad_hidden_span))
    hidden_delta = low(times_transposed(grad_hidden_span, output_delta_product))
    out_grads = low(
        transposed_times(blocked(grad_hidden_span, hidden_delta, parts), mixed_heads)
    )
    attn_delta = low(matrix_multiply(normed_span, delta_attention))
    attn_inner = low(
        times_transposed(grad_query_lin, query_delta_product)
        + times_transposed(grad_keyval, key_value_delta_product)
    )
    attn_grads = low(
        transposed_times(
            blocked(normed_span, attn_delta, parts),
            jnp.concatenate([grad_query_lin, grad_keyval, attn_inner], axis=1),
        )
    )

    def per_device(value):
        rows = value.shape[0] // parts
        return jnp.concatenate(
            [
                value[:, at : at + rank].reshape(parts, rows, rank)
                for at in range(0, value.shape[1], rank)
            ],
            axis=1,
        )

    def from_device(value, rows):
        return jnp.concatenate(
            [value[..., at : at + rows, :] for at in range(0, value.shape[-2], rows)], axis=-1
        )

    main = model_width // parts
    extra = rank // parts
    wide = main + extra
    gain_lines = jnp.stack(
        [mlp_gain_part.reshape(parts, main), attn_gain_part.reshape(parts, main)], axis=1
    )
    gain_lines = low(jnp.pad(gain_lines, ((0, 0), (0, 6), (0, rank - main))))
    head_cols = query_eff.shape[1]
    split_rows = 2 * (head_cols // rank) * wide
    first = jnp.concatenate(
        [
            per_device(out_grads),
            per_device(attn_grads),
            per_device(mlp_lora_in),
            per_device(down_lora_out),
            per_device(out_lora_out),
            gain_lines,
        ],
        axis=1,
    )
    first_sum = scattered("fsdp", first)
    split_part = first_sum[:, :split_rows]
    second_sum = scattered("tp", first_sum[:, split_rows:])[0].astype(jnp.float32)
    split_part = split_part.astype(jnp.float32)
    out_part = from_device(split_part[:, : split_rows // 2], wide)
    query_part = from_device(split_part[:, split_rows // 2 :], wide)
    sizes = [
        (keyval_eff.shape[1] // rank) * wide,
        wide,
        main,
        model_width // rank * extra,
        model_width // rank * extra,
        8,
    ]
    starts = [sum(sizes[:at]) for at in range(len(sizes))]
    pieces = [second_sum[at : at + size] for at, size in zip(starts, sizes)]
    keyval_part = from_device(pieces[0], wide)

    def rows_of(value, first_row, row_count):
        return value[:, first_row : first_row + row_count].reshape(-1, value.shape[-1])

    down_sum, gate_sum, up_sum = (
        value.astype(jnp.float32) for value in (down_sum, gate_sum, up_sum)
    )
    return (
        result,
        tokens_grad,
        pieces[5][1, :main],
        pieces[5][0, :main],
        rows_of(query_part, 0, main),
        keyval_part[:main],
        rows_of(out_part, 0, main).T,
        gate_sum[:shard_rows],
        up_sum[:shard_rows],
        down_sum[:shard_rows].T,
        pieces[1][:main],
        rows_of(query_part, main, extra),
        keyval_part[main:],
        rows_of(out_part, main, extra).T,
        from_device(pieces[4], extra),
        pieces[2],
        gate_sum[shard_rows:],
        up_sum[shard_rows:],
        down_sum[shard_rows:].T,
        from_device(pieces[3], extra),
    )


def solution(mesh):
    in_specs = (
        P(("fsdp", "tp"), None),
        P(("fsdp", "tp")),
        P(("fsdp", "tp")),
        P("fsdp", "tp"),
        P(("fsdp", "tp"), None),
        P("tp", "fsdp"),
        P("fsdp", "tp"),
        P("fsdp", "tp"),
        P("tp", "fsdp"),
        P(("fsdp", "tp"), None),
        P("fsdp", "tp"),
        P(("fsdp", "tp"), None),
        P("tp", "fsdp"),
        P(("fsdp", "tp"), None),
        P(("fsdp", "tp"), None),
        P("fsdp", "tp"),
        P("fsdp", "tp"),
        P("tp", "fsdp"),
        P(("fsdp", "tp"), None),
        P(),
        P(("fsdp", "tp"), None),
    )
    out_specs = (
        P(("fsdp", "tp"), None),
        P(("fsdp", "tp"), None),
        P(("fsdp", "tp")),
        P(("fsdp", "tp")),
        P("fsdp", "tp"),
        P(("fsdp", "tp"), None),
        P("tp", "fsdp"),
        P("fsdp", "tp"),
        P("fsdp", "tp"),
        P("tp", "fsdp"),
        P(("fsdp", "tp"), None),
        P("fsdp", "tp"),
        P(("fsdp", "tp"), None),
        P("tp", "fsdp"),
        P(("fsdp", "tp"), None),
        P(("fsdp", "tp"), None),
        P("fsdp", "tp"),
        P("fsdp", "tp"),
        P("tp", "fsdp"),
        P(("fsdp", "tp"), None),
    )
    return jax.shard_map(shards, mesh=mesh, in_specs=in_specs, out_specs=out_specs, check_vma=False)
```

```python
import jax
import jax.numpy as jnp
from jax import lax
from jax.sharding import PartitionSpec as P

HEAD_WIDTH = 256
PICTURE = 256


EPSILON = 1e-06
BLOCK_ROWS = 512


def partner(value, axis, apart):
    mask = 2**apart
    pairs = [(source, source ^ mask) for source in range(lax.axis_size(axis))]
    return lax.ppermute(value, axis, pairs)


def matrix_multiply(left_mat, right_mat):
    return jnp.dot(left_mat, right_mat, preferred_element_type=jnp.float32)


def times_transposed(left_mat, right_mat):
    return lax.dot_general(
        left_mat, right_mat, (((1,), (1,)), ((), ())), preferred_element_type=jnp.float32
    )


def transposed_times(left_mat, right_mat):
    return lax.dot_general(
        left_mat, right_mat, (((0,), (0,)), ((), ())), preferred_element_type=jnp.float32
    )


def normalize(values, gain_vec):
    return (
        values * lax.rsqrt(jnp.mean(values * values, axis=-1, keepdims=True) + EPSILON) * gain_vec
    )


def rotate(values, positions, direction):
    half_dim = HEAD_WIDTH // 2
    frequency = 10000.0 ** (-2.0 * jnp.arange(half_dim, dtype=jnp.float32) / HEAD_WIDTH)
    angles = positions.astype(jnp.float32)[:, None] * frequency[None, :]
    cosine = jnp.cos(angles)[:, None, :]
    sine_part = direction * jnp.sin(angles)[:, None, :]
    first_half = values[..., :half_dim]
    second = values[..., half_dim:]
    return jnp.concatenate(
        [first_half * cosine - second * sine_part, second * cosine + first_half * sine_part],
        axis=-1,
    )


def allowed_mask(query_pos, key_pos, picture_at):
    inside_query = (query_pos >= picture_at) & (query_pos < picture_at + PICTURE)
    inside_key = (key_pos >= picture_at) & (key_pos < picture_at + PICTURE)
    return (key_pos[None, :] <= query_pos[:, None]) | inside_query[:, None] & inside_key[None, :]


def joined(axis_names, value, axis=0):
    return lax.all_gather(value, axis_names, axis=axis, tiled=True)


def scattered(axis_names, value):
    return lax.psum_scatter(value, axis_names, scatter_dimension=0, tiled=True)


def low(value):
    return value.astype(jnp.bfloat16)


def to_lanes(value, width):
    return jnp.concatenate(
        [value[:, at : at + width] for at in range(0, value.shape[1], width)], axis=0
    )


class Packed:
    def __init__(self, width):
        self.width, self.pieces, self.shapes = width, [], []

    def add(self, value):
        self.shapes.append(value.shape)
        self.pieces.append(to_lanes(value, self.width))

    def gather(self, axis_names):
        whole = lax.all_gather(jnp.concatenate(self.pieces, axis=0), axis_names, axis=0)
        results, at = [], 0
        for rows, columns in self.shapes:
            parts = []
            for _ in range(columns // self.width):
                parts.append(whole[:, at : at + rows].reshape(-1, self.width))
                at += rows
            results.append(jnp.concatenate(parts, axis=1))
        return results


def chip_groups(fsdp_size):
    return [list(range(core, fsdp_size, 2)) for core in range(2)]


def chip_gather(value):
    fsdp_size = lax.axis_size("fsdp")
    chips = fsdp_size // 2
    if chips != 4:
        whole = lax.all_gather(value, "fsdp", axis=0, axis_index_groups=chip_groups(fsdp_size))
        return [whole[at] for at in range(chips)]
    half = value.shape[0] // 2
    along_x = partner(value, "fsdp", 1)
    along_y = partner(value, "fsdp", 2)
    far_low = partner(along_x[:half], "fsdp", 2)
    far_high = partner(along_y[half:], "fsdp", 1)
    return [value, along_x, along_y, jnp.concatenate([far_low, far_high], axis=0)]


def chip_scatter(pieces):
    fsdp_size = lax.axis_size("fsdp")
    if fsdp_size // 2 != 4:
        return lax.psum_scatter(
            jnp.concatenate(pieces, axis=0),
            "fsdp",
            scatter_dimension=0,
            tiled=True,
            axis_index_groups=chip_groups(fsdp_size),
        ).astype(jnp.float32)

    half = pieces[0].shape[1] // 2
    left = [piece[:, :half] for piece in pieces]
    right = [piece[:, half:] for piece in pieces]
    left_far = partner(left[3], "fsdp", 1)
    right_far = partner(right[3], "fsdp", 2)
    left_near = partner(left[1], "fsdp", 1)
    right_near = partner(right[2], "fsdp", 2)

    def total(*values):
        return sum(value.astype(jnp.float32) for value in values)

    left_last = partner(low(total(left[2], left_far)), "fsdp", 2)
    right_last = partner(low(total(right[1], right_far)), "fsdp", 1)
    return jnp.concatenate(
        [total(left[0], left_near, left_last), total(right[0], right_near, right_last)], axis=1
    )


def chip_relative(value, axis):
    if lax.axis_size("fsdp") // 2 != 4:
        return value
    placed = lax.axis_index("fsdp")
    size = value.shape[axis] // 4
    blocks = [lax.slice_in_dim(value, at * size, (at + 1) * size, axis=axis) for at in range(4)]
    across_x = (placed // 2) % 2 == 1
    across_y = placed // 4 == 1
    blocks = [jnp.where(across_x, blocks[at ^ 1], blocks[at]) for at in range(4)]
    blocks = [jnp.where(across_y, blocks[at ^ 2], blocks[at]) for at in range(4)]
    return jnp.concatenate(blocks, axis=axis)


def both_cores(value):
    return jnp.concatenate([value, partner(value, "fsdp", 0)], axis=0)


def core_sum(value):
    rows = value.shape[0] // 2
    return low(value[:rows] + partner(low(value[rows:]), "fsdp", 0).astype(jnp.float32))


def own_half(second, value, other=False):
    half = value.shape[1] // 2
    return jnp.where(second != other, value[:, half:], value[:, :half])


def in_order(second, mine, theirs, axis):
    return jnp.where(
        second,
        jnp.concatenate([theirs, mine], axis=axis),
        jnp.concatenate([mine, theirs], axis=axis),
    )


def tp_rows(value):
    size = lax.axis_size("tp")
    rows = value.shape[0]
    arrived = [
        lax.ppermute(value, "tp", [(at, (at + shift) % size) for at in range(size)])
        for shift in range(1, size)
    ]
    cycle = arrived[::-1] + [value] + arrived[:0:-1]
    first = (size - 1 - lax.axis_index("tp")) * rows
    return lax.dynamic_slice_in_dim(
        jnp.concatenate(cycle + [arrived[0]], axis=0), first, size * rows
    )


def gathered_wide(second, main, extra):
    shard = jnp.concatenate([main, extra], axis=0)
    theirs = partner(own_half(second, shard, True), "fsdp", 0)
    pieces = chip_gather(in_order(second, own_half(second, shard), theirs, 0))
    rows, wide = main.shape[0], shard.shape[0]
    return jnp.concatenate(
        [piece[at * wide : at * wide + rows] for piece in pieces for at in range(2)]
        + [piece[at * wide + rows : (at + 1) * wide] for piece in pieces for at in range(2)],
        axis=0,
    )


def scattered_wide(second, value, rows):
    chips = lax.axis_size("fsdp") // 2
    extra = (value.shape[0] - chips * 2 * rows) // (2 * chips)
    main_end = chips * 2 * rows
    pieces = []
    for chip in range(chips):
        for core in range(2):
            at = 2 * chip + core
            pieces.append(value[at * rows : (at + 1) * rows])
            pieces.append(value[main_end + at * extra : main_end + (at + 1) * extra])
    pieces = [jnp.concatenate(pieces[4 * at : 4 * at + 4], axis=0) for at in range(chips)]
    summed = chip_scatter(pieces)
    wide = rows + extra
    mine = jnp.where(second, summed[wide:], summed[:wide])
    theirs = partner(low(jnp.where(second, summed[:wide], summed[wide:])), "fsdp", 0)
    return in_order(second, mine, theirs.astype(jnp.float32), 1)


def shards(
    tokens,
    attention_norm_gain,
    feedforward_norm_gain,
    query_shared_weight,
    key_value_shared_weight,
    output_shared_weight,
    gate_shared_weight,
    up_shared_weight,
    down_shared_weight,
    attention_delta_input,
    query_delta_output,
    key_value_delta_output,
    output_delta_input,
    output_delta_output,
    feedforward_delta_input,
    gate_delta_output,
    up_delta_output,
    down_delta_input,
    down_delta_output,
    picture_begin_index,
    cotangent,
):
    both = ("fsdp", "tp")
    tp_size = lax.axis_size("tp")
    fsdp_size = lax.axis_size("fsdp")
    parts = tp_size * fsdp_size
    own_rows, model_width = tokens.shape
    span_rows = own_rows * tp_size
    key_rows = 2 * span_rows
    block_rows = min(BLOCK_ROWS, span_rows)
    block_count = span_rows // block_rows
    placed = lax.axis_index("fsdp")
    tp_at = lax.axis_index("tp")
    second_half = placed % 2
    picture_at = lax.dynamic_slice_in_dim(picture_begin_index, placed // 2, 1)[0]
    offset_rows = second_half * span_rows
    span_positions = offset_rows + jnp.arange(span_rows, dtype=jnp.int32)
    key_positions = jnp.arange(key_rows, dtype=jnp.int32)
    scaling = HEAD_WIDTH ** (-0.5)

    second = second_half == 1

    down_wide = gathered_wide(second, down_shared_weight.T, down_delta_input.T)
    gate_wide = gathered_wide(second, gate_shared_weight, gate_delta_output)
    up_wide = gathered_wide(second, up_shared_weight, up_delta_output)

    tokens_span = tp_rows(tokens)

    rank = gate_delta_output.shape[0] * fsdp_size
    common = Packed(rank)
    gain_rows = jnp.concatenate([attention_norm_gain[None], feedforward_norm_gain[None]], axis=0)
    common.add(jnp.pad(gain_rows, ((0, 6), (0, rank - gain_rows.shape[1]))))
    common.add(key_value_shared_weight)
    common.add(attention_delta_input)
    common.add(key_value_delta_output)
    common.add(output_delta_output)
    common.add(feedforward_delta_input)
    common.add(down_delta_output)
    (
        gains,
        key_value_complete,
        delta_attention,
        key_value_delta_product,
        output_delta_product,
        delta_feedforward,
        down_delta_product,
    ) = common.gather(both)
    gains = gains.reshape(parts, 8, rank)[:, :2, : gain_rows.shape[1]].astype(jnp.float32)
    gain_attn = gains[:, 0].reshape(-1)
    gain_mlp = gains[:, 1].reshape(-1)
    keyval_wide = jnp.concatenate([key_value_complete, key_value_delta_product], axis=0)

    head_cols = query_shared_weight.shape[1]
    shard_rows = query_shared_weight.shape[0]
    heads_stack = lax.all_gather(
        jnp.concatenate(
            [
                jnp.concatenate([query_shared_weight, output_shared_weight.T], axis=1),
                jnp.concatenate([query_delta_output, output_delta_input.T], axis=1),
            ],
            axis=0,
        ),
        "fsdp",
        axis=0,
    )
    heads_wide = jnp.concatenate(
        [
            heads_stack[:, :shard_rows].reshape(-1, 2 * head_cols),
            heads_stack[:, shard_rows:].reshape(-1, 2 * head_cols),
        ],
        axis=0,
    )
    query_wide = heads_wide[:, :head_cols]
    out_wide = heads_wide[:, head_cols:]

    grad_span = joined("tp", cotangent)
    down_delta_relative = chip_relative(down_delta_product, 0)
    grad_wide = both_cores(
        jnp.concatenate(
            [
                chip_relative(grad_span, 1),
                low(times_transposed(grad_span, down_delta_relative)),
            ],
            axis=1,
        )
    )
    down_delta_both = chip_relative(down_delta_relative, 1)
    delta_relative = chip_relative(delta_feedforward, 1)
    delta_both = chip_relative(delta_relative, 0)

    inputs = tokens.astype(jnp.float32)
    inputs_span = tokens_span.astype(jnp.float32)
    normed_span = low(normalize(inputs_span, gain_attn))
    normed_attn_wide = jnp.concatenate(
        [normed_span, low(matrix_multiply(normed_span, delta_attention))], axis=1
    )
    keyval_span = matrix_multiply(normed_attn_wide, keyval_wide)
    keys_span = rotate(keyval_span[:, None, :HEAD_WIDTH], span_positions, 1.0)[:, 0, :]
    keyval_low = low(jnp.concatenate([keys_span, keyval_span[:, HEAD_WIDTH:]], axis=1))
    keyval_other = partner(keyval_low, "fsdp", 0)
    keyval_all = jnp.where(
        second_half == 1,
        jnp.concatenate([keyval_other, keyval_low], axis=0),
        jnp.concatenate([keyval_low, keyval_other], axis=0),
    )
    keys_all = keyval_all[:, :HEAD_WIDTH]
    values_all = keyval_all[:, HEAD_WIDTH:]
    query_lin = matrix_multiply(normed_attn_wide, query_wide)
    local_heads = query_lin.shape[1] // HEAD_WIDTH
    query_rot = (
        rotate(query_lin.reshape(span_rows, local_heads, HEAD_WIDTH), span_positions, 1.0) * scaling
    )
    query_blocks = (
        low(query_rot)
        .transpose(1, 0, 2)
        .reshape(local_heads * block_count, block_rows, HEAD_WIDTH)
    )

    def block_mask(block_index):
        query_pos = (
            offset_rows
            + block_index % block_count * block_rows
            + jnp.arange(block_rows, dtype=jnp.int32)
        )
        return allowed_mask(query_pos, key_positions, picture_at)

    def attend(block_index):
        query_rows = query_blocks[block_index]
        scores = jnp.where(block_mask(block_index), times_transposed(query_rows, keys_all), -1e30)
        maximum = jnp.max(scores, axis=-1, keepdims=True)
        exponent = jnp.exp(scores - maximum)
        normalizer = jnp.sum(exponent, axis=-1, keepdims=True)
        probabilities = low(exponent / normalizer)
        return (matrix_multiply(probabilities, values_all), (maximum + jnp.log(normalizer))[:, 0])

    block_ids = jnp.arange(local_heads * block_count, dtype=jnp.int32)
    mixed_blocks, log_totals = lax.map(attend, block_ids)
    mixed_heads = low(
        mixed_blocks.reshape(local_heads, span_rows, HEAD_WIDTH)
        .transpose(1, 0, 2)
        .reshape(span_rows, local_heads * HEAD_WIDTH)
    )
    mixed_out = times_transposed(mixed_heads, out_wide)
    mixed_delta = low(mixed_out[:, model_width:])
    attn_result = scattered(
        "tp",
        low(mixed_out[:, :model_width] + matrix_multiply(mixed_delta, output_delta_product)),
    )
    hidden = inputs + attn_result.astype(jnp.float32)
    normed_own = low(normalize(hidden, gain_mlp))
    normed_wide = both_cores(
        joined(
            "tp",
            jnp.concatenate(
                [
                    chip_relative(normed_own, 1),
                    low(matrix_multiply(normed_own, delta_relative)),
                ],
                axis=1,
            ),
        )
    )

    grad_activation = matrix_multiply(grad_wide, down_wide)
    gate_lin = matrix_multiply(normed_wide, gate_wide)
    up_lin = matrix_multiply(normed_wide, up_wide)
    activation, gelu_pull = jax.vjp(
        lambda gate_vals, up_vals: jax.nn.gelu(gate_vals, approximate=True) * up_vals,
        gate_lin,
        up_lin,
    )
    activation = low(activation)
    grad_gate, grad_up = gelu_pull(grad_activation)
    grad_gate, grad_up = low(grad_gate), low(grad_up)
    grad_normed_wide = times_transposed(grad_gate, gate_wide) + times_transposed(grad_up, up_wide)
    mlp_inner = low(grad_normed_wide[:, model_width:])
    grad_normed_mlp = scattered(
        "tp",
        core_sum(
            grad_normed_wide[:, :model_width]
            + times_transposed(mlp_inner, delta_both)
        ),
    )
    grad_normed_mlp = chip_relative(grad_normed_mlp, 1).astype(jnp.float32)
    _, mlp_norm_pull = jax.vjp(normalize, hidden, gain_mlp)
    grad_hidden_norm, mlp_gain_part = mlp_norm_pull(grad_normed_mlp)
    grad_hidden = cotangent.astype(jnp.float32) + grad_hidden_norm
    grad_hidden_span = joined("tp", low(grad_hidden))

    down_sum = scattered_wide(second, low(transposed_times(grad_wide, activation)), shard_rows)
    gate_sum = scattered_wide(second, low(transposed_times(normed_wide, grad_gate)), shard_rows)
    up_sum = scattered_wide(second, low(transposed_times(normed_wide, grad_up)), shard_rows)
    mlp_lora_in = low(transposed_times(normed_wide[:, :model_width], mlp_inner))
    mlp_lora_in = chip_relative(chip_relative(mlp_lora_in, 0), 1)
    active_wide = times_transposed(activation, down_wide)
    active_delta = low(active_wide[:, model_width:])
    down_lora_out = transposed_times(active_delta, grad_wide[:, :model_width])
    down_lora_out = chip_relative(chip_relative(low(down_lora_out), 0), 1)
    mlp_result = scattered(
        "tp",
        core_sum(
            active_wide[:, :model_width]
            + matrix_multiply(active_delta, down_delta_both)
        ),
    )
    result = low(hidden + chip_relative(mlp_result, 1).astype(jnp.float32))

    grad_hidden_wide = jnp.concatenate(
        [grad_hidden_span, low(times_transposed(grad_hidden_span, output_delta_product))], axis=1
    )
    grad_mixed = low(matrix_multiply(grad_hidden_wide, out_wide))
    grad_blocks = (
        grad_mixed.reshape(span_rows, local_heads, HEAD_WIDTH)
        .transpose(1, 0, 2)
        .reshape(local_heads * block_count, block_rows, HEAD_WIDTH)
    )

    def revisit(totals, block_index):
        key_totals, value_totals = totals
        query_rows = query_blocks[block_index]
        grad_rows = grad_blocks[block_index]
        scores = jnp.where(block_mask(block_index), times_transposed(query_rows, keys_all), -1e30)
        probabilities = jnp.exp(scores - log_totals[block_index][:, None])
        grad_probs = times_transposed(grad_rows, values_all)
        inner_sum = jnp.sum(probabilities * grad_probs, axis=-1, keepdims=True)
        grad_scores = low(probabilities * (grad_probs - inner_sum))
        key_totals = key_totals + transposed_times(grad_scores, query_rows)
        value_totals = value_totals + transposed_times(low(probabilities), grad_rows)
        return ((key_totals, value_totals), matrix_multiply(grad_scores, keys_all))

    zero_rows = jnp.zeros((key_rows, HEAD_WIDTH), jnp.float32)
    (key_totals, value_totals), grad_query_blocks = lax.scan(
        revisit, (zero_rows, zero_rows), block_ids
    )
    grad_queries = (
        grad_query_blocks.reshape(local_heads, span_rows, HEAD_WIDTH).transpose(1, 0, 2) * scaling
    )
    grad_query_lin = low(
        rotate(grad_queries, span_positions, -1.0).reshape(span_rows, local_heads * HEAD_WIDTH)
    )
    keyval_totals = jnp.concatenate([key_totals, value_totals], axis=1)
    lower_rows = keyval_totals[:span_rows]
    upper_rows = keyval_totals[span_rows:]
    mine = jnp.where(second_half == 1, upper_rows, lower_rows)
    theirs = jnp.where(second_half == 1, lower_rows, upper_rows)
    keyval_part = mine + partner(theirs, "fsdp", 0)
    grad_keys = rotate(keyval_part[:, None, :HEAD_WIDTH], span_positions, -1.0)[:, 0, :]
    grad_keyval = low(jnp.concatenate([grad_keys, keyval_part[:, HEAD_WIDTH:]], axis=1))
    grad_normed_both = times_transposed(grad_query_lin, query_wide) + times_transposed(
        grad_keyval, keyval_wide
    )
    attn_inner = low(grad_normed_both[:, model_width:])
    grad_normed_part = grad_normed_both[:, :model_width] + times_transposed(
        attn_inner, delta_attention
    )
    grad_normed_attn = scattered("tp", low(grad_normed_part)).astype(jnp.float32)
    unit_span = inputs_span * lax.rsqrt(
        jnp.mean(inputs_span * inputs_span, axis=-1, keepdims=True) + EPSILON
    )
    attn_gain_part = jnp.sum(grad_normed_part * unit_span, axis=0)
    _, attn_norm_pull = jax.vjp(normalize, inputs, gain_attn)
    tokens_grad = grad_hidden + attn_norm_pull(grad_normed_attn)[0]

    out_lora_out = low(transposed_times(mixed_delta, grad_hidden_span))
    out_grads = low(transposed_times(grad_hidden_wide, mixed_heads))
    attn_grads = low(
        transposed_times(
            normed_attn_wide, jnp.concatenate([grad_query_lin, grad_keyval, attn_inner], axis=1)
        )
    )

    def per_device(value):
        rows = value.shape[0] // parts
        return jnp.concatenate(
            [
                value[:, at : at + rank].reshape(parts, rows, rank)
                for at in range(0, value.shape[1], rank)
            ],
            axis=1,
        )

    def from_device(value, rows):
        return jnp.concatenate(
            [value[..., at : at + rows, :] for at in range(0, value.shape[-2], rows)], axis=-1
        )

    def per_device_wide(value):
        return jnp.concatenate(
            [per_device(value[:model_width]), per_device(value[model_width:])], axis=1
        )

    main = model_width // parts
    extra = rank // parts
    gain_pad = ((0, 0), (0, 7), (0, rank - main))
    early = jnp.concatenate(
        [
            per_device_wide(out_grads),
            per_device(mlp_lora_in),
            per_device(down_lora_out),
            per_device(out_lora_out),
            low(jnp.pad(mlp_gain_part.reshape(parts, 1, main), gain_pad)),
        ],
        axis=1,
    )
    late = jnp.concatenate(
        [
            per_device_wide(attn_grads[:, :head_cols]),
            per_device_wide(attn_grads[:, head_cols:-rank]),
            per_device(attn_grads[:model_width, -rank:]),
            low(jnp.pad(attn_gain_part.reshape(parts, 1, main), gain_pad)),
        ],
        axis=1,
    )
    early_sum = scattered("fsdp", early)
    late_sum = scattered("fsdp", late)
    head_blocks = head_cols // rank
    keyval_blocks = keyval_wide.shape[1] // rank
    model_blocks = model_width // rank
    split_rows = head_blocks * (main + extra)
    second_sum = scattered(
        "tp", jnp.concatenate([early_sum[:, split_rows:], late_sum[:, split_rows:]], axis=1)
    )[0].astype(jnp.float32)
    out_split = early_sum[:, :split_rows].astype(jnp.float32)
    query_split = late_sum[:, :split_rows].astype(jnp.float32)
    sizes = [
        main,
        model_blocks * extra,
        model_blocks * extra,
        8,
        keyval_blocks * main,
        keyval_blocks * extra,
        main,
        8,
    ]
    starts = [sum(sizes[:at]) for at in range(len(sizes))]
    pieces = [second_sum[at : at + size] for at, size in zip(starts, sizes)]

    def split_main(value):
        return from_device(value[:, : head_blocks * main], main).reshape(-1, head_cols)

    def split_extra(value):
        return from_device(value[:, head_blocks * main :], extra).reshape(-1, head_cols)

    return (
        result,
        tokens_grad,
        pieces[7][0, :main],
        pieces[3][0, :main],
        split_main(query_split),
        from_device(pieces[4], main),
        split_main(out_split).T,
        gate_sum[:shard_rows],
        up_sum[:shard_rows],
        down_sum[:shard_rows].T,
        pieces[6],
        split_extra(query_split),
        from_device(pieces[5], extra),
        split_extra(out_split).T,
        from_device(pieces[2], extra),
        pieces[0],
        gate_sum[shard_rows:],
        up_sum[shard_rows:],
        down_sum[shard_rows:].T,
        from_device(pieces[1], extra),
    )


def solution(mesh):
    in_specs = (
        P(("fsdp", "tp"), None),
        P(("fsdp", "tp")),
        P(("fsdp", "tp")),
        P("fsdp", "tp"),
        P(("fsdp", "tp"), None),
        P("tp", "fsdp"),
        P("fsdp", "tp"),
        P("fsdp", "tp"),
        P("tp", "fsdp"),
        P(("fsdp", "tp"), None),
        P("fsdp", "tp"),
        P(("fsdp", "tp"), None),
        P("tp", "fsdp"),
        P(("fsdp", "tp"), None),
        P(("fsdp", "tp"), None),
        P("fsdp", "tp"),
        P("fsdp", "tp"),
        P("tp", "fsdp"),
        P(("fsdp", "tp"), None),
        P(),
        P(("fsdp", "tp"), None),
    )
    out_specs = (
        P(("fsdp", "tp"), None),
        P(("fsdp", "tp"), None),
        P(("fsdp", "tp")),
        P(("fsdp", "tp")),
        P("fsdp", "tp"),
        P(("fsdp", "tp"), None),
        P("tp", "fsdp"),
        P("fsdp", "tp"),
        P("fsdp", "tp"),
        P("tp", "fsdp"),
        P(("fsdp", "tp"), None),
        P("fsdp", "tp"),
        P(("fsdp", "tp"), None),
        P("tp", "fsdp"),
        P(("fsdp", "tp"), None),
        P(("fsdp", "tp"), None),
        P("fsdp", "tp"),
        P("fsdp", "tp"),
        P("tp", "fsdp"),
        P(("fsdp", "tp"), None),
    )
    return jax.shard_map(shards, mesh=mesh, in_specs=in_specs, out_specs=out_specs, check_vma=False)
```

```python
import jax
import jax.numpy as jnp
from jax import lax
from jax.sharding import PartitionSpec as P

HEAD_WIDTH = 256
PICTURE = 256


EPSILON = 1e-06
BLOCK_ROWS = 512


def partner(value, axis, apart):
    mask = 2**apart
    pairs = [(source, source ^ mask) for source in range(lax.axis_size(axis))]
    return lax.ppermute(value, axis, pairs)


def matrix_multiply(left_mat, right_mat):
    return jnp.dot(left_mat, right_mat, preferred_element_type=jnp.float32)


def times_transposed(left_mat, right_mat):
    return lax.dot_general(
        left_mat, right_mat, (((1,), (1,)), ((), ())), preferred_element_type=jnp.float32
    )


def transposed_times(left_mat, right_mat):
    return lax.dot_general(
        left_mat, right_mat, (((0,), (0,)), ((), ())), preferred_element_type=jnp.float32
    )


def normalize(values, gain_vec):
    return (
        values * lax.rsqrt(jnp.mean(values * values, axis=-1, keepdims=True) + EPSILON) * gain_vec
    )


def rotate(values, positions, direction):
    half_dim = HEAD_WIDTH // 2
    frequency = 10000.0 ** (-2.0 * jnp.arange(half_dim, dtype=jnp.float32) / HEAD_WIDTH)
    angles = positions.astype(jnp.float32)[:, None] * frequency[None, :]
    cosine = jnp.cos(angles)[:, None, :]
    sine_part = direction * jnp.sin(angles)[:, None, :]
    first_half = values[..., :half_dim]
    second = values[..., half_dim:]
    return jnp.concatenate(
        [first_half * cosine - second * sine_part, second * cosine + first_half * sine_part],
        axis=-1,
    )


def allowed_mask(query_pos, key_pos, picture_at):
    inside_query = (query_pos >= picture_at) & (query_pos < picture_at + PICTURE)
    inside_key = (key_pos >= picture_at) & (key_pos < picture_at + PICTURE)
    return (key_pos[None, :] <= query_pos[:, None]) | inside_query[:, None] & inside_key[None, :]


def joined(axis_names, value, axis=0):
    return lax.all_gather(value, axis_names, axis=axis, tiled=True)


def scattered(axis_names, value):
    return lax.psum_scatter(value, axis_names, scatter_dimension=0, tiled=True)


def low(value):
    return value.astype(jnp.bfloat16)


def to_lanes(value, width):
    return jnp.concatenate(
        [value[:, at : at + width] for at in range(0, value.shape[1], width)], axis=0
    )


class Packed:
    def __init__(self, width):
        self.width, self.pieces, self.shapes = width, [], []

    def add(self, value):
        self.shapes.append(value.shape)
        self.pieces.append(to_lanes(value, self.width))

    def gather(self, axis_names):
        stacked = jnp.concatenate(self.pieces, axis=0)
        whole = lax.all_gather(stacked, axis_names, axis=0)
        results, at = [], 0
        for rows, columns in self.shapes:
            parts = []
            for _ in range(columns // self.width):
                parts.append(whole[:, at : at + rows].reshape(-1, self.width))
                at += rows
            results.append(jnp.concatenate(parts, axis=1))
        return results


def chip_groups(fsdp_size):
    return [list(range(core, fsdp_size, 2)) for core in range(2)]


def chip_gather(value):
    fsdp_size = lax.axis_size("fsdp")
    chips = fsdp_size // 2
    if chips != 4:
        whole = lax.all_gather(value, "fsdp", axis=0, axis_index_groups=chip_groups(fsdp_size))
        return [whole[at] for at in range(chips)]
    half = value.shape[0] // 2
    along_x = partner(value, "fsdp", 1)
    along_y = partner(value, "fsdp", 2)
    far_low = partner(along_x[:half], "fsdp", 2)
    far_high = partner(along_y[half:], "fsdp", 1)
    return [value, along_x, along_y, jnp.concatenate([far_low, far_high], axis=0)]


def chip_scatter(pieces):
    fsdp_size = lax.axis_size("fsdp")
    if fsdp_size // 2 != 4:
        return lax.psum_scatter(
            jnp.concatenate(pieces, axis=0),
            "fsdp",
            scatter_dimension=0,
            tiled=True,
            axis_index_groups=chip_groups(fsdp_size),
        ).astype(jnp.float32)

    half = pieces[0].shape[1] // 2
    left = [piece[:, :half] for piece in pieces]
    right = [piece[:, half:] for piece in pieces]
    left_far = partner(left[3], "fsdp", 1)
    right_far = partner(right[3], "fsdp", 2)
    left_near = partner(left[1], "fsdp", 1)
    right_near = partner(right[2], "fsdp", 2)

    def total(*values):
        return sum(value.astype(jnp.float32) for value in values)

    left_last = partner(low(total(left[2], left_far)), "fsdp", 2)
    right_last = partner(low(total(right[1], right_far)), "fsdp", 1)
    return jnp.concatenate(
        [total(left[0], left_near, left_last), total(right[0], right_near, right_last)], axis=1
    )


def chip_relative(value, axis):
    if lax.axis_size("fsdp") // 2 != 4:
        return value
    placed = lax.axis_index("fsdp")
    size = value.shape[axis] // 4
    blocks = [lax.slice_in_dim(value, at * size, (at + 1) * size, axis=axis) for at in range(4)]
    across_x = (placed // 2) % 2 == 1
    across_y = placed // 4 == 1
    blocks = [jnp.where(across_x, blocks[at ^ 1], blocks[at]) for at in range(4)]
    blocks = [jnp.where(across_y, blocks[at ^ 2], blocks[at]) for at in range(4)]
    return jnp.concatenate(blocks, axis=axis)


def both_cores(value):
    return jnp.concatenate([value, partner(value, "fsdp", 0)], axis=0)


def core_sum(value):
    rows = value.shape[0] // 2
    return low(value[:rows] + partner(low(value[rows:]), "fsdp", 0).astype(jnp.float32))


def own_half(second, value, other=False):
    half = value.shape[1] // 2
    return jnp.where(second != other, value[:, half:], value[:, :half])


def in_order(second, mine, theirs, axis):
    return jnp.where(
        second,
        jnp.concatenate([theirs, mine], axis=axis),
        jnp.concatenate([mine, theirs], axis=axis),
    )


def tp_rows(value):
    size = lax.axis_size("tp")
    rows = value.shape[0]
    arrived = [
        lax.ppermute(value, "tp", [(at, (at + shift) % size) for at in range(size)])
        for shift in range(1, size)
    ]
    cycle = arrived[::-1] + [value] + arrived[:0:-1]
    first = (size - 1 - lax.axis_index("tp")) * rows
    return lax.dynamic_slice_in_dim(
        jnp.concatenate(cycle + [arrived[0]], axis=0), first, size * rows
    )


def gathered_wide(second, main, extra):
    shard = jnp.concatenate([main, extra], axis=0)
    theirs = partner(own_half(second, shard, True), "fsdp", 0)
    pieces = chip_gather(in_order(second, own_half(second, shard), theirs, 0))
    rows, wide = main.shape[0], shard.shape[0]
    return jnp.concatenate(
        [piece[at * wide : at * wide + rows] for piece in pieces for at in range(2)]
        + [piece[at * wide + rows : (at + 1) * wide] for piece in pieces for at in range(2)],
        axis=0,
    )


def scattered_wide(second, value, rows):
    chips = lax.axis_size("fsdp") // 2
    extra = (value.shape[0] - chips * 2 * rows) // (2 * chips)
    main_end = chips * 2 * rows
    pieces = []
    for chip in range(chips):
        for core in range(2):
            at = 2 * chip + core
            pieces.append(value[at * rows : (at + 1) * rows])
            pieces.append(value[main_end + at * extra : main_end + (at + 1) * extra])
    pieces = [jnp.concatenate(pieces[4 * at : 4 * at + 4], axis=0) for at in range(chips)]
    summed = chip_scatter(pieces)
    wide = rows + extra
    mine = jnp.where(second, summed[wide:], summed[:wide])
    theirs = partner(low(jnp.where(second, summed[:wide], summed[wide:])), "fsdp", 0)
    return in_order(second, mine, theirs.astype(jnp.float32), 1)


def shards(
    tokens,
    attention_norm_gain,
    feedforward_norm_gain,
    query_shared_weight,
    key_value_shared_weight,
    output_shared_weight,
    gate_shared_weight,
    up_shared_weight,
    down_shared_weight,
    attention_delta_input,
    query_delta_output,
    key_value_delta_output,
    output_delta_input,
    output_delta_output,
    feedforward_delta_input,
    gate_delta_output,
    up_delta_output,
    down_delta_input,
    down_delta_output,
    picture_begin_index,
    cotangent,
):
    both = ("fsdp", "tp")
    tp_size = lax.axis_size("tp")
    fsdp_size = lax.axis_size("fsdp")
    parts = tp_size * fsdp_size
    own_rows, model_width = tokens.shape
    span_rows = own_rows * tp_size
    key_rows = 2 * span_rows
    block_rows = min(BLOCK_ROWS, span_rows)
    block_count = span_rows // block_rows
    placed = lax.axis_index("fsdp")
    second_half = placed % 2
    picture_at = lax.dynamic_slice_in_dim(picture_begin_index, placed // 2, 1)[0]
    offset_rows = second_half * span_rows
    span_positions = offset_rows + jnp.arange(span_rows, dtype=jnp.int32)
    key_positions = jnp.arange(key_rows, dtype=jnp.int32)
    scaling = HEAD_WIDTH ** (-0.5)

    second = second_half == 1

    down_wide = gathered_wide(second, down_shared_weight.T, down_delta_input.T)
    gate_wide = gathered_wide(second, gate_shared_weight, gate_delta_output)
    up_wide = gathered_wide(second, up_shared_weight, up_delta_output)

    tokens_span = tp_rows(tokens)

    rank = gate_delta_output.shape[0] * fsdp_size
    common = Packed(rank)
    gain_rows = jnp.concatenate([attention_norm_gain[None], feedforward_norm_gain[None]], axis=0)
    common.add(jnp.pad(gain_rows, ((0, 6), (0, rank - gain_rows.shape[1]))))
    common.add(key_value_shared_weight)
    common.add(attention_delta_input)
    common.add(key_value_delta_output)
    common.add(output_delta_output)
    common.add(feedforward_delta_input)
    common.add(down_delta_output)
    (
        gains,
        key_value_complete,
        delta_attention,
        key_value_delta_product,
        output_delta_product,
        delta_feedforward,
        down_delta_product,
    ) = common.gather(both)
    gains = gains.reshape(parts, 8, rank)[:, :2, : gain_rows.shape[1]].astype(jnp.float32)
    gain_attn = gains[:, 0].reshape(-1)
    gain_mlp = gains[:, 1].reshape(-1)

    head_cols = query_shared_weight.shape[1]
    shard_rows = query_shared_weight.shape[0]
    heads_own = jnp.concatenate(
        [
            jnp.concatenate([query_shared_weight, output_shared_weight.T], axis=1),
            jnp.concatenate([query_delta_output, output_delta_input.T], axis=1),
        ],
        axis=0,
    )
    heads_stack = lax.all_gather(heads_own, "fsdp", axis=0)
    heads_main = heads_stack[:, :shard_rows].reshape(-1, 2 * head_cols)
    heads_delta = heads_stack[:, shard_rows:].reshape(-1, 2 * head_cols)
    query_delta_product, out_delta_in = heads_delta[:, :head_cols], heads_delta[:, head_cols:]
    query_eff = low(
        heads_main[:, :head_cols].astype(jnp.float32)
        + matrix_multiply(delta_attention, query_delta_product)
    )
    out_eff = low(
        heads_main[:, head_cols:].astype(jnp.float32)
        + transposed_times(output_delta_product, out_delta_in)
    )
    keyval_eff = low(
        key_value_complete.astype(jnp.float32)
        + matrix_multiply(delta_attention, key_value_delta_product)
    )

    grad_span = joined("tp", cotangent)
    down_delta_relative = chip_relative(down_delta_product, 0)
    grad_wide = both_cores(
        jnp.concatenate(
            [
                chip_relative(grad_span, 1),
                low(times_transposed(grad_span, down_delta_relative)),
            ],
            axis=1,
        )
    )
    down_delta_both = chip_relative(down_delta_relative, 1)
    delta_relative = chip_relative(delta_feedforward, 1)
    delta_both = chip_relative(delta_relative, 0)

    inputs = tokens.astype(jnp.float32)
    inputs_span = tokens_span.astype(jnp.float32)
    normed_span = low(normalize(inputs_span, gain_attn))
    keyval_span = matrix_multiply(normed_span, keyval_eff)
    keys_span = rotate(keyval_span[:, None, :HEAD_WIDTH], span_positions, 1.0)[:, 0, :]
    keyval_low = low(jnp.concatenate([keys_span, keyval_span[:, HEAD_WIDTH:]], axis=1))
    keyval_other = partner(keyval_low, "fsdp", 0)
    keyval_all = jnp.where(
        second_half == 1,
        jnp.concatenate([keyval_other, keyval_low], axis=0),
        jnp.concatenate([keyval_low, keyval_other], axis=0),
    )
    keys_all = keyval_all[:, :HEAD_WIDTH]
    values_all = keyval_all[:, HEAD_WIDTH:]
    query_lin = matrix_multiply(normed_span, query_eff)
    local_heads = query_lin.shape[1] // HEAD_WIDTH
    query_rot = (
        rotate(query_lin.reshape(span_rows, local_heads, HEAD_WIDTH), span_positions, 1.0) * scaling
    )
    query_blocks = (
        low(query_rot)
        .transpose(1, 0, 2)
        .reshape(local_heads * block_count, block_rows, HEAD_WIDTH)
    )

    def block_mask(block_index):
        query_pos = (
            offset_rows
            + block_index % block_count * block_rows
            + jnp.arange(block_rows, dtype=jnp.int32)
        )
        return allowed_mask(query_pos, key_positions, picture_at)

    def attend(block_index):
        query_rows = query_blocks[block_index]
        scores = jnp.where(block_mask(block_index), times_transposed(query_rows, keys_all), -1e30)
        maximum = jnp.max(scores, axis=-1, keepdims=True)
        exponent = jnp.exp(scores - maximum)
        normalizer = jnp.sum(exponent, axis=-1, keepdims=True)
        probabilities = low(exponent / normalizer)
        return (matrix_multiply(probabilities, values_all), (maximum + jnp.log(normalizer))[:, 0])

    block_ids = jnp.arange(local_heads * block_count, dtype=jnp.int32)
    mixed_blocks, log_totals = lax.map(attend, block_ids)
    mixed_heads = low(
        mixed_blocks.reshape(local_heads, span_rows, HEAD_WIDTH)
        .transpose(1, 0, 2)
        .reshape(span_rows, local_heads * HEAD_WIDTH)
    )
    mixed_out = low(times_transposed(mixed_heads, out_eff))
    attn_result = scattered("tp", mixed_out)
    hidden = inputs + attn_result.astype(jnp.float32)
    normed_own = low(normalize(hidden, gain_mlp))
    normed_wide = jnp.concatenate(
        [chip_relative(normed_own, 1), low(matrix_multiply(normed_own, delta_relative))], axis=1
    )
    normed_wide = joined("tp", normed_wide)
    normed_wide = both_cores(normed_wide)

    grad_activation = matrix_multiply(grad_wide, down_wide)
    gate_lin = matrix_multiply(normed_wide, gate_wide)
    up_lin = matrix_multiply(normed_wide, up_wide)
    activation, gelu_pull = jax.vjp(
        lambda gate_vals, up_vals: jax.nn.gelu(gate_vals, approximate=True) * up_vals,
        gate_lin,
        up_lin,
    )
    activation = low(activation)
    grad_gate, grad_up = gelu_pull(grad_activation)
    grad_gate, grad_up = low(grad_gate), low(grad_up)
    grad_normed_wide = times_transposed(grad_gate, gate_wide) + times_transposed(grad_up, up_wide)
    mlp_inner = low(grad_normed_wide[:, model_width:])
    grad_normed_mlp = core_sum(
        grad_normed_wide[:, :model_width] + times_transposed(mlp_inner, delta_both)
    )
    grad_normed_mlp = scattered("tp", grad_normed_mlp)
    grad_normed_mlp = chip_relative(grad_normed_mlp, 1).astype(jnp.float32)
    _, mlp_norm_pull = jax.vjp(normalize, hidden, gain_mlp)
    grad_hidden_norm, mlp_gain_part = mlp_norm_pull(grad_normed_mlp)
    grad_hidden = cotangent.astype(jnp.float32) + grad_hidden_norm
    grad_hidden_span = joined("tp", low(grad_hidden))

    down_grads = low(transposed_times(grad_wide, activation))
    gate_grads = low(transposed_times(normed_wide, grad_gate))
    up_grads = low(transposed_times(normed_wide, grad_up))
    down_sum = scattered_wide(second, down_grads, shard_rows)
    gate_sum = scattered_wide(second, gate_grads, shard_rows)
    up_sum = scattered_wide(second, up_grads, shard_rows)
    mlp_lora_in = low(transposed_times(normed_wide[:, :model_width], mlp_inner))
    mlp_lora_in = chip_relative(chip_relative(mlp_lora_in, 0), 1)
    active_wide = times_transposed(activation, down_wide)
    active_delta = low(active_wide[:, model_width:])
    down_lora_out = transposed_times(active_delta, grad_wide[:, :model_width])
    down_lora_out = chip_relative(chip_relative(low(down_lora_out), 0), 1)
    mlp_result = core_sum(
        active_wide[:, :model_width] + matrix_multiply(active_delta, down_delta_both)
    )
    mlp_result = scattered("tp", mlp_result)
    result = low(hidden + chip_relative(mlp_result, 1).astype(jnp.float32))

    grad_hidden_wide = jnp.concatenate(
        [grad_hidden_span, low(times_transposed(grad_hidden_span, output_delta_product))], axis=1
    )
    grad_mixed = low(matrix_multiply(grad_hidden_span, out_eff))
    grad_blocks = (
        grad_mixed.reshape(span_rows, local_heads, HEAD_WIDTH)
        .transpose(1, 0, 2)
        .reshape(local_heads * block_count, block_rows, HEAD_WIDTH)
    )

    def revisit(totals, block_index):
        key_totals, value_totals = totals
        query_rows = query_blocks[block_index]
        grad_rows = grad_blocks[block_index]
        scores = jnp.where(block_mask(block_index), times_transposed(query_rows, keys_all), -1e30)
        probabilities = jnp.exp(scores - log_totals[block_index][:, None])
        grad_probs = times_transposed(grad_rows, values_all)
        inner_sum = jnp.sum(probabilities * grad_probs, axis=-1, keepdims=True)
        grad_scores = low(probabilities * (grad_probs - inner_sum))
        key_totals = key_totals + transposed_times(grad_scores, query_rows)
        value_totals = value_totals + transposed_times(low(probabilities), grad_rows)
        return ((key_totals, value_totals), matrix_multiply(grad_scores, keys_all))

    zero_rows = jnp.zeros((key_rows, HEAD_WIDTH), jnp.float32)
    (key_totals, value_totals), grad_query_blocks = lax.scan(
        revisit, (zero_rows, zero_rows), block_ids
    )
    grad_queries = (
        grad_query_blocks.reshape(local_heads, span_rows, HEAD_WIDTH).transpose(1, 0, 2) * scaling
    )
    grad_query_lin = low(
        rotate(grad_queries, span_positions, -1.0).reshape(span_rows, local_heads * HEAD_WIDTH)
    )
    keyval_totals = jnp.concatenate([key_totals, value_totals], axis=1)
    lower_rows = keyval_totals[:span_rows]
    upper_rows = keyval_totals[span_rows:]
    mine = jnp.where(second_half == 1, upper_rows, lower_rows)
    theirs = jnp.where(second_half == 1, lower_rows, upper_rows)
    keyval_part = mine + partner(theirs, "fsdp", 0)
    grad_keys = rotate(keyval_part[:, None, :HEAD_WIDTH], span_positions, -1.0)[:, 0, :]
    grad_keyval = low(jnp.concatenate([grad_keys, keyval_part[:, HEAD_WIDTH:]], axis=1))
    grad_normed_part = times_transposed(grad_query_lin, query_eff) + times_transposed(
        grad_keyval, keyval_eff
    )
    attn_inner = low(
        times_transposed(grad_query_lin, query_delta_product)
        + times_transposed(grad_keyval, key_value_delta_product)
    )
    grad_normed_attn = scattered("tp", low(grad_normed_part)).astype(jnp.float32)
    unit_span = inputs_span * lax.rsqrt(
        jnp.mean(inputs_span * inputs_span, axis=-1, keepdims=True) + EPSILON
    )
    attn_gain_part = jnp.sum(grad_normed_part * unit_span, axis=0)
    _, attn_norm_pull = jax.vjp(normalize, inputs, gain_attn)
    tokens_grad = grad_hidden + attn_norm_pull(grad_normed_attn)[0]

    normed_attn_wide = jnp.concatenate(
        [normed_span, low(matrix_multiply(normed_span, delta_attention))], axis=1
    )
    mixed_delta = low(times_transposed(mixed_heads, out_delta_in))
    out_lora_out = low(transposed_times(mixed_delta, grad_hidden_span))
    out_grads = low(transposed_times(grad_hidden_wide, mixed_heads))
    attn_grads = low(
        transposed_times(
            normed_attn_wide, jnp.concatenate([grad_query_lin, grad_keyval, attn_inner], axis=1)
        )
    )

    def per_device(value):
        rows = value.shape[0] // parts
        return jnp.concatenate(
            [
                value[:, at : at + rank].reshape(parts, rows, rank)
                for at in range(0, value.shape[1], rank)
            ],
            axis=1,
        )

    def from_device(value, rows):
        return jnp.concatenate(
            [value[..., at : at + rows, :] for at in range(0, value.shape[-2], rows)], axis=-1
        )

    def per_device_wide(value):
        return jnp.concatenate(
            [per_device(value[:model_width]), per_device(value[model_width:])], axis=1
        )

    main = model_width // parts
    extra = rank // parts
    gain_pad = ((0, 0), (0, 7), (0, rank - main))
    early = jnp.concatenate(
        [
            per_device_wide(out_grads),
            per_device(mlp_lora_in),
            per_device(down_lora_out),
            per_device(out_lora_out),
            low(jnp.pad(mlp_gain_part.reshape(parts, 1, main), gain_pad)),
        ],
        axis=1,
    )
    late = jnp.concatenate(
        [
            per_device_wide(attn_grads[:, :head_cols]),
            per_device_wide(attn_grads[:, head_cols:-rank]),
            per_device(attn_grads[:model_width, -rank:]),
            low(jnp.pad(attn_gain_part.reshape(parts, 1, main), gain_pad)),
        ],
        axis=1,
    )
    early_sum = scattered("fsdp", early)
    late_sum = scattered("fsdp", late)
    head_blocks = head_cols // rank
    keyval_blocks = keyval_eff.shape[1] // rank
    model_blocks = model_width // rank
    split_rows = head_blocks * (main + extra)
    second_sum = scattered(
        "tp", jnp.concatenate([early_sum[:, split_rows:], late_sum[:, split_rows:]], axis=1)
    )[0].astype(jnp.float32)
    out_split = early_sum[:, :split_rows].astype(jnp.float32)
    query_split = late_sum[:, :split_rows].astype(jnp.float32)
    sizes = [
        main,
        model_blocks * extra,
        model_blocks * extra,
        8,
        keyval_blocks * main,
        keyval_blocks * extra,
        main,
        8,
    ]
    starts = [sum(sizes[:at]) for at in range(len(sizes))]
    pieces = [second_sum[at : at + size] for at, size in zip(starts, sizes)]

    def split_main(value):
        return from_device(value[:, : head_blocks * main], main).reshape(-1, head_cols)

    def split_extra(value):
        return from_device(value[:, head_blocks * main :], extra).reshape(-1, head_cols)

    return (
        result,
        tokens_grad,
        pieces[7][0, :main],
        pieces[3][0, :main],
        split_main(query_split),
        from_device(pieces[4], main),
        split_main(out_split).T,
        gate_sum[:shard_rows],
        up_sum[:shard_rows],
        down_sum[:shard_rows].T,
        pieces[6],
        split_extra(query_split),
        from_device(pieces[5], extra),
        split_extra(out_split).T,
        from_device(pieces[2], extra),
        pieces[0],
        gate_sum[shard_rows:],
        up_sum[shard_rows:],
        down_sum[shard_rows:].T,
        from_device(pieces[1], extra),
    )


def solution(mesh):
    in_specs = (
        P(("fsdp", "tp"), None),
        P(("fsdp", "tp")),
        P(("fsdp", "tp")),
        P("fsdp", "tp"),
        P(("fsdp", "tp"), None),
        P("tp", "fsdp"),
        P("fsdp", "tp"),
        P("fsdp", "tp"),
        P("tp", "fsdp"),
        P(("fsdp", "tp"), None),
        P("fsdp", "tp"),
        P(("fsdp", "tp"), None),
        P("tp", "fsdp"),
        P(("fsdp", "tp"), None),
        P(("fsdp", "tp"), None),
        P("fsdp", "tp"),
        P("fsdp", "tp"),
        P("tp", "fsdp"),
        P(("fsdp", "tp"), None),
        P(),
        P(("fsdp", "tp"), None),
    )
    out_specs = (
        P(("fsdp", "tp"), None),
        P(("fsdp", "tp"), None),
        P(("fsdp", "tp")),
        P(("fsdp", "tp")),
        P("fsdp", "tp"),
        P(("fsdp", "tp"), None),
        P("tp", "fsdp"),
        P("fsdp", "tp"),
        P("fsdp", "tp"),
        P("tp", "fsdp"),
        P(("fsdp", "tp"), None),
        P("fsdp", "tp"),
        P(("fsdp", "tp"), None),
        P("tp", "fsdp"),
        P(("fsdp", "tp"), None),
        P(("fsdp", "tp"), None),
        P("fsdp", "tp"),
        P("fsdp", "tp"),
        P("tp", "fsdp"),
        P(("fsdp", "tp"), None),
    )

    return jax.shard_map(shards, mesh=mesh, in_specs=in_specs, out_specs=out_specs, check_vma=False)
```

```python
import jax
import jax.numpy as jnp
from jax import lax
from jax.sharding import PartitionSpec as P

HEAD_WIDTH = 256
PICTURE = 256


EPSILON = 1e-06
BLOCK_ROWS = 512


def partner(value, axis, apart):
    mask = 2**apart
    pairs = [(source, source ^ mask) for source in range(lax.axis_size(axis))]
    return lax.ppermute(value, axis, pairs)


def matrix_multiply(left_mat, right_mat):
    return jnp.dot(left_mat, right_mat, preferred_element_type=jnp.float32)


def times_transposed(left_mat, right_mat):
    return lax.dot_general(
        left_mat, right_mat, (((1,), (1,)), ((), ())), preferred_element_type=jnp.float32
    )


def transposed_times(left_mat, right_mat):
    return lax.dot_general(
        left_mat, right_mat, (((0,), (0,)), ((), ())), preferred_element_type=jnp.float32
    )


def normalize(values, gain_vec):
    return (
        values * lax.rsqrt(jnp.mean(values * values, axis=-1, keepdims=True) + EPSILON) * gain_vec
    )


def rotate(values, positions, direction):
    half_dim = HEAD_WIDTH // 2
    frequency = 10000.0 ** (-2.0 * jnp.arange(half_dim, dtype=jnp.float32) / HEAD_WIDTH)
    angles = positions.astype(jnp.float32)[:, None] * frequency[None, :]
    cosine = jnp.cos(angles)[:, None, :]
    sine_part = direction * jnp.sin(angles)[:, None, :]
    first_half = values[..., :half_dim]
    second = values[..., half_dim:]
    return jnp.concatenate(
        [first_half * cosine - second * sine_part, second * cosine + first_half * sine_part],
        axis=-1,
    )


def allowed_mask(query_pos, key_pos, picture_at):
    inside_query = (query_pos >= picture_at) & (query_pos < picture_at + PICTURE)
    inside_key = (key_pos >= picture_at) & (key_pos < picture_at + PICTURE)
    return (key_pos[None, :] <= query_pos[:, None]) | inside_query[:, None] & inside_key[None, :]


def joined(axis_names, value, axis=0):
    return lax.all_gather(value, axis_names, axis=axis, tiled=True)


def scattered(axis_names, value):
    return lax.psum_scatter(value, axis_names, scatter_dimension=0, tiled=True)


def low(value):
    return value.astype(jnp.bfloat16)


def to_lanes(value, width):
    return jnp.concatenate(
        [value[:, at : at + width] for at in range(0, value.shape[1], width)], axis=0
    )


class Packed:
    def __init__(self, width):
        self.width, self.pieces, self.shapes = width, [], []

    def add(self, value):
        self.shapes.append(value.shape)
        self.pieces.append(to_lanes(value, self.width))

    def gather(self, axis_names):
        stacked = jnp.concatenate(self.pieces, axis=0)
        whole = lax.all_gather(stacked, axis_names, axis=0)
        results, at = [], 0
        for rows, columns in self.shapes:
            parts = []
            for _ in range(columns // self.width):
                parts.append(whole[:, at : at + rows].reshape(-1, self.width))
                at += rows
            results.append(jnp.concatenate(parts, axis=1))
        return results


def chip_groups(fsdp_size):
    return [list(range(core, fsdp_size, 2)) for core in range(2)]


def chip_gather(value):
    fsdp_size = lax.axis_size("fsdp")
    chips = fsdp_size // 2
    if chips != 4:
        whole = lax.all_gather(value, "fsdp", axis=0, axis_index_groups=chip_groups(fsdp_size))
        return [[whole[at]] for at in range(chips)]
    half = value.shape[0] // 2
    along_x = partner(value, "fsdp", 1)
    along_y = partner(value, "fsdp", 2)
    far_low = partner(along_x[:half], "fsdp", 2)
    far_high = partner(along_y[half:], "fsdp", 1)
    return [[value], [along_x], [along_y], [far_low, far_high]]


def chip_scatter(pieces):
    fsdp_size = lax.axis_size("fsdp")
    if fsdp_size // 2 != 4:
        return lax.psum_scatter(
            jnp.concatenate(pieces, axis=0),
            "fsdp",
            scatter_dimension=0,
            tiled=True,
            axis_index_groups=chip_groups(fsdp_size),
        ).astype(jnp.float32)

    half = pieces[0].shape[1] // 2
    left = [piece[:, :half] for piece in pieces]
    right = [piece[:, half:] for piece in pieces]
    left_far = partner(left[3], "fsdp", 1)
    right_far = partner(right[3], "fsdp", 2)
    left_near = partner(left[1], "fsdp", 1)
    right_near = partner(right[2], "fsdp", 2)

    def total(*values):
        return sum(value.astype(jnp.float32) for value in values)

    left_last = partner(low(total(left[2], left_far)), "fsdp", 2)
    right_last = partner(low(total(right[1], right_far)), "fsdp", 1)
    return jnp.concatenate(
        [total(left[0], left_near, left_last), total(right[0], right_near, right_last)], axis=1
    )


def chip_relative(value, axis):
    if lax.axis_size("fsdp") // 2 != 4:
        return value
    placed = lax.axis_index("fsdp")
    size = value.shape[axis] // 4
    blocks = [lax.slice_in_dim(value, at * size, (at + 1) * size, axis=axis) for at in range(4)]
    across_x = (placed // 2) % 2 == 1
    across_y = placed // 4 == 1
    blocks = [jnp.where(across_x, blocks[at ^ 1], blocks[at]) for at in range(4)]
    blocks = [jnp.where(across_y, blocks[at ^ 2], blocks[at]) for at in range(4)]
    return jnp.concatenate(blocks, axis=axis)


def both_cores(value):
    return jnp.concatenate([value, partner(value, "fsdp", 0)], axis=0)


def core_sum(value):
    rows = value.shape[0] // 2
    return low(value[:rows] + partner(low(value[rows:]), "fsdp", 0).astype(jnp.float32))


def own_half(second, value, other=False):
    half = value.shape[1] // 2
    return jnp.where(second != other, value[:, half:], value[:, :half])


def in_order(second, mine, theirs, axis):
    return jnp.where(
        second,
        jnp.concatenate([theirs, mine], axis=axis),
        jnp.concatenate([mine, theirs], axis=axis),
    )


def tp_rows(value):
    size = lax.axis_size("tp")
    rows = value.shape[0]
    arrived = [
        lax.ppermute(value, "tp", [(at, (at + shift) % size) for at in range(size)])
        for shift in range(1, size)
    ]
    cycle = arrived[::-1] + [value] + arrived[:0:-1]
    first = (size - 1 - lax.axis_index("tp")) * rows
    return lax.dynamic_slice_in_dim(
        jnp.concatenate(cycle + [arrived[0]], axis=0), first, size * rows
    )


def row_parts(pieces, first, last):
    parts, start = [], 0
    for piece in pieces:
        low_row, high_row = max(first - start, 0), min(last - start, piece.shape[0])
        if low_row < high_row:
            parts.append(piece[low_row:high_row])
        start += piece.shape[0]
    return parts


def gathered_wide(second, main, extra):
    rows = main.shape[0]
    shard = jnp.concatenate([main, extra], axis=0)
    mine = own_half(second, shard)
    theirs = partner(own_half(second, shard, True), "fsdp", 0)
    block = jnp.where(
        second,
        jnp.concatenate([theirs[:rows], mine[:rows], theirs[rows:], mine[rows:]], axis=0),
        jnp.concatenate([mine[:rows], theirs[:rows], mine[rows:], theirs[rows:]], axis=0),
    )
    pieces = chip_gather(block)
    wide = []
    for first, last in ((0, 2 * rows), (2 * rows, block.shape[0])):
        for piece in pieces:
            wide += row_parts(piece, first, last)
    return jnp.concatenate(wide, axis=0)


def scattered_wide(second, value, rows):
    chips = lax.axis_size("fsdp") // 2
    main_end = chips * 2 * rows
    extra = (value.shape[0] - main_end) // (2 * chips)
    pieces = [
        jnp.concatenate(
            [
                value[2 * at * rows : 2 * (at + 1) * rows],
                value[main_end + 2 * at * extra : main_end + 2 * (at + 1) * extra],
            ],
            axis=0,
        )
        for at in range(chips)
    ]
    summed = chip_scatter(pieces)
    first = jnp.concatenate([summed[:rows], summed[2 * rows : 2 * rows + extra]], axis=0)
    other = jnp.concatenate([summed[rows : 2 * rows], summed[2 * rows + extra :]], axis=0)
    sent = low(jnp.where(second, first, other))
    theirs = partner(sent, "fsdp", 0)
    return in_order(second, jnp.where(second, other, first), theirs.astype(jnp.float32), 1)


def device_sum(value):
    fsdp_size = lax.axis_size("fsdp")
    tp_size = lax.axis_size("tp")
    if fsdp_size != 8:
        return scattered("fsdp", value).astype(jnp.float32)
    placed = lax.axis_index("fsdp")
    rows, width = value.shape[1:]
    value = value.reshape(4, 2, tp_size * rows, width)
    mine = lax.dynamic_index_in_dim(value, placed % 2, 1, keepdims=False)
    got = partner(
        lax.dynamic_index_in_dim(value, 1 - placed % 2, 1, keepdims=False), "fsdp", 0
    )
    chip_sums = low(mine.astype(jnp.float32) + got.astype(jnp.float32))
    pieces = [
        lax.dynamic_index_in_dim(chip_sums, (placed // 2) ^ at, 0, keepdims=False)
        for at in range(4)
    ]
    return chip_scatter(pieces).reshape(tp_size, rows, width)


def shards(
    tokens,
    attention_norm_gain,
    feedforward_norm_gain,
    query_shared_weight,
    key_value_shared_weight,
    output_shared_weight,
    gate_shared_weight,
    up_shared_weight,
    down_shared_weight,
    attention_delta_input,
    query_delta_output,
    key_value_delta_output,
    output_delta_input,
    output_delta_output,
    feedforward_delta_input,
    gate_delta_output,
    up_delta_output,
    down_delta_input,
    down_delta_output,
    picture_begin_index,
    cotangent,
):
    both = ("fsdp", "tp")
    tp_size = lax.axis_size("tp")
    fsdp_size = lax.axis_size("fsdp")
    parts = tp_size * fsdp_size
    own_rows, model_width = tokens.shape
    span_rows = own_rows * tp_size
    key_rows = 2 * span_rows
    block_rows = min(BLOCK_ROWS, span_rows)
    block_count = span_rows // block_rows
    placed = lax.axis_index("fsdp")
    second_half = placed % 2
    picture_at = lax.dynamic_slice_in_dim(picture_begin_index, placed // 2, 1)[0]
    offset_rows = second_half * span_rows
    span_positions = offset_rows + jnp.arange(span_rows, dtype=jnp.int32)
    key_positions = jnp.arange(key_rows, dtype=jnp.int32)
    scaling = HEAD_WIDTH ** (-0.5)

    second = second_half == 1

    down_wide = gathered_wide(second, down_shared_weight.T, down_delta_input.T)
    gate_wide = gathered_wide(second, gate_shared_weight, gate_delta_output)
    up_wide = gathered_wide(second, up_shared_weight, up_delta_output)

    tokens_span = tp_rows(tokens)

    rank = gate_delta_output.shape[0] * fsdp_size
    common = Packed(rank)
    gain_rows = jnp.concatenate([attention_norm_gain[None], feedforward_norm_gain[None]], axis=0)
    common.add(jnp.pad(gain_rows, ((0, 6), (0, rank - gain_rows.shape[1]))))
    common.add(key_value_shared_weight)
    common.add(attention_delta_input)
    common.add(key_value_delta_output)
    (gains, key_value_complete, delta_attention, key_value_delta_product) = common.gather(both)
    extra = output_delta_output.shape[0]
    lanes = [
        feedforward_delta_input[at * extra : (at + 1) * extra] for at in range(model_width // rank)
    ]
    extra_own = jnp.concatenate(
        [output_delta_output, down_delta_output, jnp.concatenate(lanes, axis=1)], axis=0
    )
    extra_stack = lax.all_gather(extra_own, both, axis=0)
    output_delta_product = extra_stack[:, :extra].reshape(rank, model_width)
    down_delta_product = extra_stack[:, extra : 2 * extra].reshape(rank, model_width)
    delta_feedforward = jnp.concatenate(
        [
            extra_stack[:, 2 * extra :, at : at + rank]
            for at in range(0, model_width, rank)
        ],
        axis=1,
    ).reshape(model_width, rank)
    gains = gains.reshape(parts, 8, rank)[:, :2, : gain_rows.shape[1]].astype(jnp.float32)
    gain_attn = gains[:, 0].reshape(-1)
    gain_mlp = gains[:, 1].reshape(-1)

    head_cols = query_shared_weight.shape[1]
    shard_rows = query_shared_weight.shape[0]
    heads_own = jnp.concatenate(
        [
            jnp.concatenate([query_shared_weight, output_shared_weight.T], axis=1),
            jnp.concatenate([query_delta_output, output_delta_input.T], axis=1),
        ],
        axis=0,
    )
    heads_stack = lax.all_gather(heads_own, "fsdp", axis=0)
    heads_main = heads_stack[:, :shard_rows].reshape(-1, 2 * head_cols)
    heads_delta = heads_stack[:, shard_rows:].reshape(-1, 2 * head_cols)
    query_delta_product, out_delta_in = heads_delta[:, :head_cols], heads_delta[:, head_cols:]
    query_eff = low(
        heads_main[:, :head_cols].astype(jnp.float32)
        + matrix_multiply(delta_attention, query_delta_product)
    )
    out_eff = low(
        heads_main[:, head_cols:].astype(jnp.float32)
        + transposed_times(output_delta_product, out_delta_in)
    )
    keyval_eff = low(
        key_value_complete.astype(jnp.float32)
        + matrix_multiply(delta_attention, key_value_delta_product)
    )

    grad_span = tp_rows(cotangent)
    down_delta_relative = chip_relative(down_delta_product, 0)
    grad_wide = both_cores(
        jnp.concatenate(
            [
                chip_relative(grad_span, 1),
                low(times_transposed(grad_span, down_delta_relative)),
            ],
            axis=1,
        )
    )
    down_delta_both = chip_relative(down_delta_relative, 1)
    delta_relative = chip_relative(delta_feedforward, 1)
    delta_both = chip_relative(delta_relative, 0)

    inputs = tokens.astype(jnp.float32)
    inputs_span = tokens_span.astype(jnp.float32)
    normed_span = low(normalize(inputs_span, gain_attn))
    keyval_span = matrix_multiply(normed_span, keyval_eff)
    keys_span = rotate(keyval_span[:, None, :HEAD_WIDTH], span_positions, 1.0)[:, 0, :]
    keyval_low = low(jnp.concatenate([keys_span, keyval_span[:, HEAD_WIDTH:]], axis=1))
    keyval_other = partner(keyval_low, "fsdp", 0)
    keyval_all = jnp.where(
        second_half == 1,
        jnp.concatenate([keyval_other, keyval_low], axis=0),
        jnp.concatenate([keyval_low, keyval_other], axis=0),
    )
    keys_all = keyval_all[:, :HEAD_WIDTH]
    values_all = keyval_all[:, HEAD_WIDTH:]
    query_lin = matrix_multiply(normed_span, query_eff)
    local_heads = query_lin.shape[1] // HEAD_WIDTH
    query_rot = (
        rotate(query_lin.reshape(span_rows, local_heads, HEAD_WIDTH), span_positions, 1.0) * scaling
    )
    query_blocks = (
        low(query_rot)
        .transpose(1, 0, 2)
        .reshape(local_heads * block_count, block_rows, HEAD_WIDTH)
    )

    def block_mask(block_index):
        query_pos = (
            offset_rows
            + block_index % block_count * block_rows
            + jnp.arange(block_rows, dtype=jnp.int32)
        )
        return allowed_mask(query_pos, key_positions, picture_at)

    def attend(block_index):
        query_rows = query_blocks[block_index]
        scores = jnp.where(block_mask(block_index), times_transposed(query_rows, keys_all), -1e30)
        maximum = jnp.max(scores, axis=-1, keepdims=True)
        exponent = jnp.exp(scores - maximum)
        normalizer = jnp.sum(exponent, axis=-1, keepdims=True)
        probabilities = low(exponent / normalizer)
        return (matrix_multiply(probabilities, values_all), (maximum + jnp.log(normalizer))[:, 0])

    block_ids = jnp.arange(local_heads * block_count, dtype=jnp.int32)
    mixed_blocks, log_totals = lax.map(attend, block_ids)
    mixed_heads = low(
        mixed_blocks.reshape(local_heads, span_rows, HEAD_WIDTH)
        .transpose(1, 0, 2)
        .reshape(span_rows, local_heads * HEAD_WIDTH)
    )
    mixed_out = low(times_transposed(mixed_heads, out_eff))
    attn_result = scattered("tp", mixed_out)
    hidden = inputs + attn_result.astype(jnp.float32)
    normed_own = low(normalize(hidden, gain_mlp))
    normed_delta = low(matrix_multiply(normed_own, delta_relative))
    normed_wide = jnp.concatenate([chip_relative(normed_own, 1), normed_delta], axis=1)
    normed_wide = joined("tp", normed_wide)
    normed_wide = both_cores(normed_wide)

    grad_activation = matrix_multiply(grad_wide, down_wide)
    gate_lin = matrix_multiply(normed_wide, gate_wide)
    up_lin = matrix_multiply(normed_wide, up_wide)
    activation, gelu_pull = jax.vjp(
        lambda gate_vals, up_vals: jax.nn.gelu(gate_vals, approximate=True) * up_vals,
        gate_lin,
        up_lin,
    )
    activation = low(activation)
    grad_gate, grad_up = gelu_pull(grad_activation)
    grad_gate, grad_up = low(grad_gate), low(grad_up)
    grad_normed_wide = times_transposed(grad_gate, gate_wide) + times_transposed(grad_up, up_wide)
    mlp_inner = low(grad_normed_wide[:, model_width:])
    grad_normed_mlp = core_sum(
        grad_normed_wide[:, :model_width] + times_transposed(mlp_inner, delta_both)
    )
    grad_normed_mlp = scattered("tp", grad_normed_mlp)
    grad_normed_mlp = chip_relative(grad_normed_mlp, 1).astype(jnp.float32)
    _, mlp_norm_pull = jax.vjp(normalize, hidden, gain_mlp)
    grad_hidden_norm, mlp_gain_part = mlp_norm_pull(grad_normed_mlp)
    grad_hidden = cotangent.astype(jnp.float32) + grad_hidden_norm
    grad_hidden_span = joined("tp", low(grad_hidden))

    down_grads = low(transposed_times(grad_wide, activation))
    gate_grads = low(transposed_times(normed_wide, grad_gate))
    up_grads = low(transposed_times(normed_wide, grad_up))
    down_sum = scattered_wide(second, down_grads, shard_rows)
    gate_sum = scattered_wide(second, gate_grads, shard_rows)
    up_sum = scattered_wide(second, up_grads, shard_rows)
    mlp_lora_in = low(transposed_times(normed_wide[:, :model_width], mlp_inner))
    mlp_lora_in = chip_relative(chip_relative(mlp_lora_in, 0), 1)
    active_wide = times_transposed(activation, down_wide)
    active_delta = low(active_wide[:, model_width:])
    down_lora_out = transposed_times(active_delta, grad_wide[:, :model_width])
    down_lora_out = chip_relative(chip_relative(low(down_lora_out), 0), 1)
    mlp_result = core_sum(
        active_wide[:, :model_width] + matrix_multiply(active_delta, down_delta_both)
    )
    mlp_result = scattered("tp", mlp_result)
    result = low(hidden + chip_relative(mlp_result, 1).astype(jnp.float32))

    grad_hidden_wide = jnp.concatenate(
        [grad_hidden_span, low(times_transposed(grad_hidden_span, output_delta_product))], axis=1
    )
    grad_mixed = low(matrix_multiply(grad_hidden_span, out_eff))
    grad_blocks = (
        grad_mixed.reshape(span_rows, local_heads, HEAD_WIDTH)
        .transpose(1, 0, 2)
        .reshape(local_heads * block_count, block_rows, HEAD_WIDTH)
    )

    def revisit(totals, block_index):
        key_totals, value_totals = totals
        query_rows = query_blocks[block_index]
        grad_rows = grad_blocks[block_index]
        scores = jnp.where(block_mask(block_index), times_transposed(query_rows, keys_all), -1e30)
        probabilities = jnp.exp(scores - log_totals[block_index][:, None])
        grad_probs = times_transposed(grad_rows, values_all)
        inner_sum = jnp.sum(probabilities * grad_probs, axis=-1, keepdims=True)
        grad_scores = low(probabilities * (grad_probs - inner_sum))
        key_totals = key_totals + transposed_times(grad_scores, query_rows)
        value_totals = value_totals + transposed_times(low(probabilities), grad_rows)
        return ((key_totals, value_totals), matrix_multiply(grad_scores, keys_all))

    zero_rows = jnp.zeros((key_rows, HEAD_WIDTH), jnp.float32)
    (key_totals, value_totals), grad_query_blocks = lax.scan(
        revisit, (zero_rows, zero_rows), block_ids
    )
    grad_queries = (
        grad_query_blocks.reshape(local_heads, span_rows, HEAD_WIDTH).transpose(1, 0, 2) * scaling
    )
    grad_query_lin = low(
        rotate(grad_queries, span_positions, -1.0).reshape(span_rows, local_heads * HEAD_WIDTH)
    )
    keyval_totals = jnp.concatenate([key_totals, value_totals], axis=1)
    lower_rows = keyval_totals[:span_rows]
    upper_rows = keyval_totals[span_rows:]
    mine = jnp.where(second_half == 1, upper_rows, lower_rows)
    theirs = jnp.where(second_half == 1, lower_rows, upper_rows)
    keyval_part = mine + partner(theirs, "fsdp", 0)
    grad_keys = rotate(keyval_part[:, None, :HEAD_WIDTH], span_positions, -1.0)[:, 0, :]
    grad_keyval = low(jnp.concatenate([grad_keys, keyval_part[:, HEAD_WIDTH:]], axis=1))
    grad_normed_part = times_transposed(grad_query_lin, query_eff) + times_transposed(
        grad_keyval, keyval_eff
    )
    attn_inner = low(
        times_transposed(grad_query_lin, query_delta_product)
        + times_transposed(grad_keyval, key_value_delta_product)
    )
    grad_normed_attn = scattered("tp", low(grad_normed_part)).astype(jnp.float32)
    unit_span = inputs_span * lax.rsqrt(
        jnp.mean(inputs_span * inputs_span, axis=-1, keepdims=True) + EPSILON
    )
    attn_gain_part = jnp.sum(grad_normed_part * unit_span, axis=0)
    _, attn_norm_pull = jax.vjp(normalize, inputs, gain_attn)
    tokens_grad = grad_hidden + attn_norm_pull(grad_normed_attn)[0]

    normed_attn_wide = jnp.concatenate(
        [normed_span, low(matrix_multiply(normed_span, delta_attention))], axis=1
    )
    mixed_delta = low(times_transposed(mixed_heads, out_delta_in))
    out_lora_out = low(transposed_times(mixed_delta, grad_hidden_span))
    out_grads = low(transposed_times(grad_hidden_wide, mixed_heads))
    attn_grads = low(
        transposed_times(
            normed_attn_wide, jnp.concatenate([grad_query_lin, grad_keyval, attn_inner], axis=1)
        )
    )

    def per_device(value):
        rows = value.shape[0] // parts
        return jnp.concatenate(
            [
                value[:, at : at + rank].reshape(parts, rows, rank)
                for at in range(0, value.shape[1], rank)
            ],
            axis=1,
        )

    def from_device(value, rows):
        return jnp.concatenate(
            [value[..., at : at + rows, :] for at in range(0, value.shape[-2], rows)], axis=-1
        )

    def per_device_wide(value):
        return jnp.concatenate(
            [per_device(value[:model_width]), per_device(value[model_width:])], axis=1
        )

    main = model_width // parts
    extra = rank // parts
    gain_pad = ((0, 0), (0, 7), (0, rank - main))
    early = jnp.concatenate(
        [
            per_device_wide(out_grads),
            per_device(mlp_lora_in),
            per_device(down_lora_out),
            per_device(out_lora_out),
            low(jnp.pad(mlp_gain_part.reshape(parts, 1, main), gain_pad)),
        ],
        axis=1,
    )
    late = jnp.concatenate(
        [
            per_device_wide(attn_grads[:, :head_cols]),
            per_device_wide(attn_grads[:, head_cols:-rank]),
            per_device(attn_grads[:model_width, -rank:]),
            low(jnp.pad(attn_gain_part.reshape(parts, 1, main), gain_pad)),
        ],
        axis=1,
    )
    early_sum = device_sum(early)
    late_sum = device_sum(late)
    head_blocks = head_cols // rank
    keyval_blocks = keyval_eff.shape[1] // rank
    model_blocks = model_width // rank
    split_rows = head_blocks * (main + extra)
    second_sum = scattered(
        "tp", low(jnp.concatenate([early_sum[:, split_rows:], late_sum[:, split_rows:]], axis=1))
    )[0].astype(jnp.float32)
    out_split = early_sum[:, :split_rows]
    query_split = late_sum[:, :split_rows]
    sizes = [
        main,
        model_blocks * extra,
        model_blocks * extra,
        8,
        keyval_blocks * main,
        keyval_blocks * extra,
        main,
        8,
    ]
    starts = [sum(sizes[:at]) for at in range(len(sizes))]
    pieces = [second_sum[at : at + size] for at, size in zip(starts, sizes)]

    def split_main(value):
        return from_device(value[:, : head_blocks * main], main).reshape(-1, head_cols)

    def split_extra(value):
        return from_device(value[:, head_blocks * main :], extra).reshape(-1, head_cols)

    return (
        result,
        tokens_grad,
        pieces[7][0, :main],
        pieces[3][0, :main],
        split_main(query_split),
        from_device(pieces[4], main),
        split_main(out_split).T,
        gate_sum[:shard_rows],
        up_sum[:shard_rows],
        down_sum[:shard_rows].T,
        pieces[6],
        split_extra(query_split),
        from_device(pieces[5], extra),
        split_extra(out_split).T,
        from_device(pieces[2], extra),
        pieces[0],
        gate_sum[shard_rows:],
        up_sum[shard_rows:],
        down_sum[shard_rows:].T,
        from_device(pieces[1], extra),
    )


def solution(mesh):
    in_specs = (
        P(("fsdp", "tp"), None),
        P(("fsdp", "tp")),
        P(("fsdp", "tp")),
        P("fsdp", "tp"),
        P(("fsdp", "tp"), None),
        P("tp", "fsdp"),
        P("fsdp", "tp"),
        P("fsdp", "tp"),
        P("tp", "fsdp"),
        P(("fsdp", "tp"), None),
        P("fsdp", "tp"),
        P(("fsdp", "tp"), None),
        P("tp", "fsdp"),
        P(("fsdp", "tp"), None),
        P(("fsdp", "tp"), None),
        P("fsdp", "tp"),
        P("fsdp", "tp"),
        P("tp", "fsdp"),
        P(("fsdp", "tp"), None),
        P(),
        P(("fsdp", "tp"), None),
    )
    out_specs = (
        P(("fsdp", "tp"), None),
        P(("fsdp", "tp"), None),
        P(("fsdp", "tp")),
        P(("fsdp", "tp")),
        P("fsdp", "tp"),
        P(("fsdp", "tp"), None),
        P("tp", "fsdp"),
        P("fsdp", "tp"),
        P("fsdp", "tp"),
        P("tp", "fsdp"),
        P(("fsdp", "tp"), None),
        P("fsdp", "tp"),
        P(("fsdp", "tp"), None),
        P("tp", "fsdp"),
        P(("fsdp", "tp"), None),
        P(("fsdp", "tp"), None),
        P("fsdp", "tp"),
        P("fsdp", "tp"),
        P("tp", "fsdp"),
        P(("fsdp", "tp"), None),
    )

    return jax.shard_map(shards, mesh=mesh, in_specs=in_specs, out_specs=out_specs, check_vma=False)
```
